768 devices in a mesh: dc: 64 (over x, y, core), tp: 12 (over z).
Axes of the slice: x: 4, y: 8, z: 12, core: 2. Of those that a mesh axis runs over, the one named last changes fastest.
Arguments:
- queries: bfloat16 [12288, 3072], P('dc', 'tp'), may hold values from -15 to 15
- keys: bfloat16 [12288, 768], P('dc'), may hold values from -4.5 to 4.5
- values: bfloat16 [12288, 768], P('dc'), may hold values from -5 to 5
- lengths: int32 [24], replicated, may hold values from 1 to 9216, 12288 in all
- mlp_owner: int32 [12288], replicated, may hold values from 0 to 63, as said below
- out_weight: bfloat16 [3072, 4096], P('tp'), may hold values from -0.109375 to 0.109375
- residual: bfloat16 [12288, 4096], P(('dc', 'tp')), may hold values from -3 to 3
Outputs:
- hidden: bfloat16 [12288, 4096], P(('dc', 'tp'))
The draws below stay inside these ranges and needn't reach their ends.
Inputs may be any that keep to these rules, and one draw needn't show every extreme that they name: `mlp_owner`: the tokens of any one slab of 192 positions send at most 6 tokens to one owner, and every owner receives exactly 192 tokens.
All inputs are finite; a program needn't handle non-finite values.
Results may differ from the reference program's by a relative error of at most 0.013.
Values may be sent and summed in bfloat16 or wider, within the bound.
No kernel may reach another device: no remote copies, remote signals or barrier semaphores. Data moves between devices by JAX's collectives and lax.ppermute only.
A program may use at most 128 MiB of HBM per device.

```python
import math
import jax
import jax.numpy as jnp
import numpy as np
from jax import lax

D = 4096
HEAD_SIZE = 128
GROUP = 4
DOCS = 24
TOK_DEV = 192
HQ = 24
KEY_VALUE_HEADS = 6
ROW_TOKENS = 12288
MOST = 9216
N_DC = 64


def draw_queries(key, part):
    normal_key = jax.random.fold_in(jax.random.fold_in(key, 1), 0)
    base_offset = jax.random.normal(normal_key, (ROW_TOKENS, HQ * HEAD_SIZE), jnp.float32) * 3.0
    base_offset = jnp.clip(base_offset, -15.0, 15.0)
    return base_offset.astype(jnp.bfloat16)


def draw_keys(key, part):
    base_offset = jax.random.normal(jax.random.fold_in(key, 2), (ROW_TOKENS, KEY_VALUE_HEADS * HEAD_SIZE), jnp.float32)
    base_offset = jnp.clip(base_offset, -4.5, 4.5)
    return base_offset.astype(jnp.bfloat16)


def draw_mlp_owner(key, part):
    perm_key, shuffle_key = jax.random.split(jax.random.fold_in(key, 3))
    owners = jnp.arange(N_DC, dtype=jnp.int32)
    source = owners[:, None]
    target = owners[None, :]
    remainder = TOK_DEV % N_DC
    counts = TOK_DEV // N_DC + ((target - source) % N_DC < remainder).astype(jnp.int32)
    mapping = jax.random.permutation(perm_key, N_DC).astype(jnp.int32)
    first = (target == mapping[:, None]).astype(jnp.int32)
    second = (target == (mapping[:, None] + 1) % N_DC).astype(jnp.int32)
    counts = counts + TOK_DEV // N_DC * (first - second)
    labels = jax.vmap(lambda row: jnp.repeat(owners, row, total_repeat_length=TOK_DEV))(counts)
    shuffle_keys = jax.random.split(shuffle_key, N_DC)
    mixed = jax.vmap(lambda single, row: jax.random.permutation(single, row))(shuffle_keys, labels)
    return mixed.reshape(ROW_TOKENS).astype(jnp.int32)


def shard_levels(key, extent, pieces, least, largest):
    loudness = 1.0
    for axis_at, blocks in pieces:
        steps = jax.random.uniform(jax.random.fold_in(jax.random.fold_in(key, 6), axis_at), (blocks,), jnp.float32, least / len(pieces), largest / len(pieces))
        loudness = loudness * jnp.repeat(jnp.exp(steps), extent[axis_at] // blocks).reshape((-1,) + (1,) * (len(extent) - 1 - axis_at))
    return loudness


def length_profile(amount, total, reach, skew):
    portions = [(1 << 20) // math.isqrt(rank ** skew) + 1 for rank in range(2, amount + 1)]
    rest, given = total - reach - (amount - 1), [1] * (amount - 1)
    while rest > 0:
        free = [i for i in range(amount - 1) if given[i] < reach]
        mass, remaining = sum([portions[i] for i in free]), rest
        for i in free:
            more = min(reach - given[i], max(1, remaining * portions[i] // mass), rest)
            given[i] = given[i] + more
            rest = rest - more
    return np.array([reach] + given)


def ragged(rng, count, total, reach, slope):
    if count == 2:
        one = jax.random.randint(rng, (), max(1, total - reach), min(reach, total - 1) + 1)
        return jnp.stack([one, total - one])
    sizes = jnp.asarray(length_profile(count, total, reach, slope), jnp.int32)
    couples = (count - 1) // 2
    donor, sink = sizes[1:1 + 2 * couples:2], sizes[2:2 + 2 * couples:2]
    slack = jnp.minimum(donor - 1, reach - sink)
    moved = jax.random.randint(jax.random.fold_in(rng, 1), (couples,), 0, 1 << 20) % (slack + 1)
    sizes = sizes.at[1:1 + 2 * couples:2].set(donor - moved).at[2:2 + 2 * couples:2].set(sink + moved)
    return sizes[jax.random.permutation(jax.random.fold_in(rng, 2), count)]


def centred(own_key, extent, scale, most, shards=(), held_as=jnp.bfloat16):
    entries = jax.random.normal(own_key, extent, jnp.float32) * scale
    if len(shards) > 0:
        entries = shard_levels(own_key, extent, shards, -0.22, 0.18) * entries
    return jnp.clip(entries, min=-most, max=most).astype(held_as)


def setup_inputs(seed: int = 0) -> dict:
    splits = jax.random.split(jax.random.key(seed), 8)
    queries = draw_queries(jax.random.fold_in(splits[7], 71), 0)
    keys = draw_keys(jax.random.fold_in(splits[7], 71), 0)
    values = centred(splits[2], (ROW_TOKENS, KEY_VALUE_HEADS * HEAD_SIZE), 1.0, 5.0, ((0, 64),))
    lengths = ragged(splits[3], DOCS, ROW_TOKENS, MOST, 2).astype(jnp.int32)
    mlp_owner = draw_mlp_owner(jax.random.fold_in(splits[7], 71), 0)
    out_weight = centred(splits[5], (HQ * HEAD_SIZE, D), (HQ * HEAD_SIZE) ** -0.5, 0.109375, ((0, 12),))
    residual = centred(splits[6], (ROW_TOKENS, D), 0.5, 3.0, ((0, 768),))
    return dict(queries=queries, keys=keys, values=values, lengths=lengths, mlp_owner=mlp_owner, out_weight=out_weight, residual=residual)


def doc_index(positions, doc_ends):
    return jnp.sum((positions[:, None] >= doc_ends[None, :]).astype(jnp.int32), axis=1)


def reference(queries, keys, values, lengths, mlp_owner, out_weight, residual):
    doc_ends = jnp.cumsum(lengths).astype(jnp.int32)
    positions = jnp.arange(ROW_TOKENS, dtype=jnp.int32)
    documents = doc_index(positions, doc_ends)
    block_rows = math.gcd(ROW_TOKENS, 512)
    block_total = ROW_TOKENS // block_rows
    scale = HEAD_SIZE ** -0.5

    def one_head(head):
        query_cols = lax.dynamic_slice_in_dim(queries, head * HEAD_SIZE, HEAD_SIZE, 1)
        shared = head // GROUP
        key_cols = lax.dynamic_slice_in_dim(keys, shared * HEAD_SIZE, HEAD_SIZE, 1)
        value_cols = lax.dynamic_slice_in_dim(values, shared * HEAD_SIZE, HEAD_SIZE, 1)

        def one_block(block):
            offset = block * block_rows
            query_rows = lax.dynamic_slice_in_dim(query_cols, offset, block_rows, 0)
            query_pos = offset + jnp.arange(block_rows, dtype=jnp.int32)
            query_doc = lax.dynamic_slice_in_dim(documents, offset, block_rows, 0)
            allowed = (documents[None, :] == query_doc[:, None]) & (positions[None, :] <= query_pos[:, None])
            scores = jnp.dot(query_rows, key_cols.T, preferred_element_type=jnp.float32) * scale
            scores = jnp.where(allowed, scores, -1e30)
            highest = jnp.max(scores, axis=1, keepdims=True)
            weights = jnp.where(allowed, jnp.exp(scores - highest), 0.0)
            total = jnp.sum(weights, axis=1, keepdims=True)
            mixed = jnp.dot(weights.astype(jnp.bfloat16), value_cols, preferred_element_type=jnp.float32)
            return mixed / total

        return lax.map(one_block, jnp.arange(block_total, dtype=jnp.int32)).reshape(ROW_TOKENS, HEAD_SIZE)

    per_head = lax.map(one_head, jnp.arange(HQ, dtype=jnp.int32))
    attention = jnp.transpose(per_head, (1, 0, 2)).reshape(ROW_TOKENS, HQ * HEAD_SIZE).astype(jnp.bfloat16)
    ordering = jnp.argsort(mlp_owner, stable=True)
    routed = attention[ordering]
    projected = jnp.dot(routed, out_weight, preferred_element_type=jnp.float32)
    return (projected + residual.astype(jnp.float32)).astype(jnp.bfloat16)
```

```python
import jax
import jax.numpy as jnp
from jax import lax
from jax.experimental import pallas as pl
from jax.experimental.pallas import tpu as pltpu
from jax.sharding import Mesh, PartitionSpec as P

HEAD = 128
GROUP = 4
NX, NY, NC, NQ, NJ = 4, 8, 2, 4, 3
TOK = 192
DOCS = 24
HEADS_HERE = 2
COLS = HEADS_HERE * HEAD
QROWS = HEADS_HERE * TOK
SLOTS = 6
N_DC = NX * NY * NC
SLOT_TOTAL = N_DC * SLOTS
CHUNK_SLABS = 4
CHUNK = CHUNK_SLABS * TOK
PART = HEAD + 16
LOG2E = 1.4426950408889634
SCALE2 = HEAD**-0.5 * LOG2E
NEG = -1e30
FLOOR = -1e9


NT = (((1,), (1,)), ((), ()))
TN = (((0,), (0,)), ((), ()))


def round_up(v):
    return (v + jnp.abs(v) * 0.0079).astype(jnp.bfloat16).astype(jnp.float32)


def attend_kernel(place, lengths, q_ref, own_ref, peer_ref, out_ref, q_s, m_s, l_s, acc_s):
    x, y, c = place[0], place[1], place[2]

    def empty(xs, carry):
        out_ref[xs, :HEAD, :] = jnp.zeros((HEAD, QROWS), jnp.bfloat16)
        rows = lax.broadcasted_iota(jnp.int32, (PART - HEAD, QROWS), 0)
        out_ref[xs, HEAD:, :] = jnp.where(rows == 0, FLOOR, 0.0).astype(jnp.bfloat16)
        return carry

    lax.fori_loop(0, x, empty, 0)

    def slab(xs, carry):
        p0 = (xs * (NY * NC) + y * NC + c) * TOK
        last = p0 + TOK - 1
        lane = lax.broadcasted_iota(jnp.int32, (1, QROWS), 1)
        pos = p0 + jnp.where(lane >= TOK, lane - TOK, lane)
        start = jnp.zeros((1, QROWS), jnp.int32)
        first_start = jnp.int32(0)
        last_start = jnp.int32(0)
        end = jnp.int32(0)
        for k in range(DOCS):
            end = end + lengths[k]
            start = jnp.where(pos >= end, end, start)
            first_start = jnp.where(p0 >= end, end, first_start)
            last_start = jnp.where(last >= end, end, last_start)
        q_s[:TOK, :] = q_ref[xs, :, :HEAD]
        q_s[TOK:, :] = q_ref[xs, :, HEAD:]
        m_s[...] = jnp.full((1, QROWS), FLOOR, jnp.float32)
        l_s[...] = jnp.zeros((1, QROWS), jnp.float32)
        acc_s[...] = jnp.zeros((HEAD, QROWS), jnp.float32)

        for ref, core in ((own_ref, c), (peer_ref, 1 - c)):

            def chunk(ch, carry, ref=ref, core=core):
                low = ((x * NY + ch * CHUNK_SLABS) * NC + core) * TOK
                high = low + (CHUNK_SLABS - 1) * NC * TOK + TOK - 1
                rows = pl.ds(pl.multiple_of(ch * CHUNK, CHUNK), CHUNK)

                def update(masked):
                    s = lax.dot_general(
                        ref[rows, :HEAD], q_s[...], NT, preferred_element_type=jnp.float32
                    )
                    s = s * SCALE2
                    if masked:
                        at = lax.broadcasted_iota(jnp.int32, (CHUNK, 1), 0)
                        slab_at = jnp.zeros((CHUNK, 1), jnp.int32)
                        for n in range(1, CHUNK_SLABS):
                            slab_at += (at >= n * TOK).astype(jnp.int32)
                        key_pos = low + at + slab_at * ((NC - 1) * TOK)
                        s = jnp.where((key_pos >= start) & (key_pos <= pos), s, NEG)
                    m_old = m_s[...]
                    m_new = jnp.maximum(m_old, round_up(jnp.max(s, axis=0, keepdims=True)))
                    w = jnp.exp2(s - m_new)
                    fix = jnp.exp2(m_old - m_new)
                    m_s[...] = m_new
                    l_s[...] = l_s[...] * fix + jnp.sum(w, axis=0, keepdims=True)
                    acc_s[...] = acc_s[...] * fix + lax.dot_general(
                        ref[rows, HEAD:],
                        w.astype(jnp.bfloat16),
                        TN,
                        preferred_element_type=jnp.float32,
                    )

                needed = (low <= last) & (high >= first_start)
                whole = (high <= p0) & (low >= last_start)

                @pl.when(needed & whole)
                def _():
                    update(False)

                @pl.when(needed & jnp.logical_not(whole))
                def _():
                    update(True)

                return carry

            lax.fori_loop(0, NY // CHUNK_SLABS, chunk, 0)

        out_ref[xs, :HEAD, :] = acc_s[...].astype(jnp.bfloat16)
        total = l_s[...]
        high_part = total.astype(jnp.bfloat16).astype(jnp.float32)
        rows = lax.broadcasted_iota(jnp.int32, (PART - HEAD, QROWS), 0)
        stats = jnp.where(rows == 0, m_s[...], jnp.where(rows == 1, high_part, total - high_part))
        out_ref[xs, HEAD:, :] = stats.astype(jnp.bfloat16)
        return carry

    lax.fori_loop(x, NX, slab, 0)


def merge_kernel(part_ref, row_ref, col_ref, out_ref):
    m = [part_ref[i, HEAD : HEAD + 1, :].astype(jnp.float32) for i in range(NX)]
    top = jnp.maximum(jnp.maximum(m[0], m[1]), jnp.maximum(m[2], m[3]))
    total = jnp.zeros((1, QROWS), jnp.float32)
    mixed = jnp.zeros((HEAD, QROWS), jnp.float32)
    for i in range(NX):
        w = jnp.exp2(m[i] - top)
        part = part_ref[i, HEAD + 1 : HEAD + 2, :].astype(jnp.float32)
        part = part + part_ref[i, HEAD + 2 : HEAD + 3, :].astype(jnp.float32)
        total = total + w * part
        mixed = mixed + w * part_ref[i, :HEAD, :].astype(jnp.float32)
    attention = (mixed / total).astype(jnp.bfloat16)
    target = row_ref[...]
    earlier = lax.broadcasted_iota(jnp.int32, (TOK, TOK), 0) < lax.broadcasted_iota(
        jnp.int32, (TOK, TOK), 1
    )
    same = (col_ref[...] == target) & earlier
    rank = jnp.sum(same.astype(jnp.int32), axis=0, keepdims=True)
    slot = target * SLOTS + rank
    ids = lax.broadcasted_iota(jnp.int32, (SLOT_TOTAL, TOK), 0)
    placement = (ids == slot).astype(jnp.float32).astype(jnp.bfloat16)
    for h in range(HEADS_HERE):
        out_ref[:, h * HEAD : (h + 1) * HEAD] = lax.dot_general(
            placement,
            attention[:, h * TOK : (h + 1) * TOK],
            NT,
            preferred_element_type=jnp.float32,
        ).astype(jnp.bfloat16)


def collect_kernel(me, owner_ref, in_ref, out_ref):
    mine = (owner_ref[...] == me[0]).astype(jnp.float32).astype(jnp.bfloat16)
    count = lax.dot_general(
        jnp.ones((8, TOK), jnp.bfloat16), mine, NT, preferred_element_type=jnp.float32
    ).astype(jnp.bfloat16)
    before = lax.broadcasted_iota(jnp.int32, (N_DC, N_DC), 0) < lax.broadcasted_iota(
        jnp.int32, (N_DC, N_DC), 1
    )
    first = jnp.dot(
        count, before.astype(jnp.float32).astype(jnp.bfloat16), preferred_element_type=jnp.float32
    ).astype(jnp.bfloat16)
    src = lax.broadcasted_iota(jnp.int32, (N_DC, SLOT_TOTAL), 0)
    slot = lax.broadcasted_iota(jnp.int32, (N_DC, SLOT_TOTAL), 1)
    inside = (slot >= src * SLOTS) & (slot < (src + 1) * SLOTS)
    spread = inside.astype(jnp.float32).astype(jnp.bfloat16)
    count = jnp.dot(count, spread, preferred_element_type=jnp.float32)[:1]
    first = jnp.dot(first, spread, preferred_element_type=jnp.float32)[:1]
    k = (slot[:1] % SLOTS).astype(jnp.float32)
    g = jnp.where(k < count, first + k, -1.0).astype(jnp.int32)
    at = lax.broadcasted_iota(jnp.int32, (TOK, 1), 0)
    part = (at >= 64).astype(jnp.int32) + (at >= 128).astype(jnp.int32)
    within = at - 64 * part
    wanted = ((within // 16) * NJ + part) * 16 + within % 16
    chooser = (g == wanted).astype(jnp.float32).astype(jnp.bfloat16)
    out_ref[...] = jnp.dot(chooser, in_ref[...], preferred_element_type=jnp.float32).astype(
        jnp.bfloat16
    )


def project_kernel(place, x_ref, w0, a1, a2, b1, b2, out_ref):
    c, j = place[0], place[1]
    total = jnp.dot(x_ref[j], w0[...], preferred_element_type=jnp.float32)
    for step, near, far in ((1, a1, b1), (2, a2, b2)):
        rows = x_ref[lax.rem(j + NJ - step, NJ)]
        left, right = rows[:, :HEAD], rows[:, HEAD:]
        lo = jnp.where(c == 0, left, right)
        hi = jnp.where(c == 0, right, left)
        total += jnp.dot(lo, near[...], preferred_element_type=jnp.float32)
        total += jnp.dot(hi, far[...], preferred_element_type=jnp.float32)
    out_ref[...] = total.astype(jnp.bfloat16)


def vmem():
    return pl.BlockSpec(memory_space=pltpu.VMEM)


def smem():
    return pl.BlockSpec(memory_space=pltpu.SMEM)


def per_device(queries, keys, values, lengths, mlp_owner, out_weight, residual):
    x, y, c = lax.axis_index("x"), lax.axis_index("y"), lax.axis_index("c")
    j = lax.axis_index("j")
    tp = lax.axis_index("q") * NJ + j
    dc = (x * NY + y) * NC + c
    place = jnp.stack([x, y, c]).astype(jnp.int32)
    peer = [(0, 1), (1, 0)]

    half = lax.dynamic_slice_in_dim(out_weight, c * HEAD, HEAD, 0)
    near = [lax.ppermute(half, "j", [(i, (i + s) % NJ) for i in range(NJ)]) for s in (1, 2)]
    far = [lax.ppermute(w, "c", peer) for w in near]

    kv_at = tp * HEADS_HERE // GROUP * HEAD
    kv = jnp.concatenate(
        [
            lax.dynamic_slice_in_dim(keys, kv_at, HEAD, 1),
            lax.dynamic_slice_in_dim(values, kv_at, HEAD, 1),
        ],
        axis=1,
    )
    own = lax.all_gather(kv, "y", axis=0, tiled=True)
    other = lax.ppermute(own, "c", peer)
    q_all = lax.all_gather(queries, "x", axis=0, tiled=False)

    partial = pl.pallas_call(
        attend_kernel,
        out_shape=jax.ShapeDtypeStruct((NX, PART, QROWS), jnp.bfloat16),
        in_specs=[smem(), smem(), vmem(), vmem(), vmem()],
        out_specs=vmem(),
        scratch_shapes=[
            pltpu.VMEM((QROWS, HEAD), jnp.bfloat16),
            pltpu.VMEM((1, QROWS), jnp.float32),
            pltpu.VMEM((1, QROWS), jnp.float32),
            pltpu.VMEM((HEAD, QROWS), jnp.float32),
        ],
        name="attend",
    )(place, lengths, q_all, own, other)
    parts = lax.all_to_all(partial, "x", 0, 0, tiled=True)

    targets = lax.dynamic_slice_in_dim(mlp_owner, dc * TOK, TOK, 0)
    outgoing = pl.pallas_call(
        merge_kernel,
        out_shape=jax.ShapeDtypeStruct((SLOT_TOTAL, COLS), jnp.bfloat16),
        in_specs=[vmem(), vmem(), vmem()],
        out_specs=vmem(),
        name="merge",
    )(parts, targets.reshape(1, TOK), targets.reshape(TOK, 1))
    incoming = lax.all_to_all(
        outgoing.reshape(N_DC, SLOTS, COLS), ("x", "y", "c"), 0, 0, tiled=True
    )
    owned = pl.pallas_call(
        collect_kernel,
        out_shape=jax.ShapeDtypeStruct((TOK, COLS), jnp.bfloat16),
        in_specs=[smem(), vmem(), vmem()],
        out_specs=vmem(),
        name="collect",
    )(
        dc.reshape(1).astype(jnp.int32),
        mlp_owner.reshape(N_DC, TOK),
        incoming.reshape(SLOT_TOTAL, COLS),
    )
    shared = lax.all_to_all(owned.reshape(NJ, TOK // NJ, COLS), "j", 0, 0, tiled=True)

    width = out_weight.shape[1]
    tile = 1024
    rows = TOK // NJ
    projected = pl.pallas_call(
        project_kernel,
        out_shape=jax.ShapeDtypeStruct((rows, width), jnp.bfloat16),
        grid=(width // tile,),
        in_specs=[
            smem(),
            pl.BlockSpec((NJ, rows, COLS), lambda n: (0, 0, 0)),
            pl.BlockSpec((COLS, tile), lambda n: (0, n)),
            pl.BlockSpec((HEAD, tile), lambda n: (0, n)),
            pl.BlockSpec((HEAD, tile), lambda n: (0, n)),
            pl.BlockSpec((HEAD, tile), lambda n: (0, n)),
            pl.BlockSpec((HEAD, tile), lambda n: (0, n)),
        ],
        out_specs=pl.BlockSpec((rows, tile), lambda n: (0, n)),
        name="project",
    )(jnp.stack([c, j]).astype(jnp.int32), shared, out_weight, near[0], near[1], far[0], far[1])
    tiles = lax.all_to_all(projected.reshape(NQ, rows // NQ, width), "q", 0, 0, tiled=True)
    summed = jnp.sum(tiles.astype(jnp.float32), axis=0)
    return (summed + residual.astype(jnp.float32)).astype(jnp.bfloat16)


def solution(mesh):
    fine = Mesh(mesh.devices.reshape(NX, NY, NC, NQ, NJ), ("x", "y", "c", "q", "j"))
    dcs, tps = ("x", "y", "c"), ("q", "j")
    return jax.shard_map(
        per_device,
        mesh=fine,
        in_specs=(
            P(dcs, tps),
            P(dcs, None),
            P(dcs, None),
            P(),
            P(),
            P(tps, None),
            P(dcs + tps, None),
        ),
        out_specs=P(dcs + tps, None),
        check_vma=False,
    )
```

```python
import jax
import jax.numpy as jnp
from jax import lax
from jax.experimental import pallas as pl
from jax.experimental.pallas import tpu as pltpu
from jax.sharding import Mesh, PartitionSpec as P

HEAD = 128
GROUP = 4
NX, NY, NC, NQ, NJ = 4, 8, 2, 4, 3
TOK = 192
DOCS = 24
HEADS_HERE = 2
COLS = HEADS_HERE * HEAD
QROWS = HEADS_HERE * TOK
SLOTS = 6
N_DC = NX * NY * NC
SLOT_TOTAL = N_DC * SLOTS
CHUNK_SLABS = 4
CHUNK = CHUNK_SLABS * TOK
PART = HEAD + 16
LOG2E = 1.4426950408889634
SCALE2 = HEAD**-0.5 * LOG2E
NEG = -1e30
FLOOR = -1e9


NT = (((1,), (1,)), ((), ()))
TN = (((0,), (0,)), ((), ()))


def round_up(v):
    return (v + jnp.abs(v) * 0.0079).astype(jnp.bfloat16).astype(jnp.float32)


def attend_kernel(place, lengths, q_ref, own_ref, peer_ref, out_ref, q_s, m_s, l_s, acc_s):
    x, y, c = place[0], place[1], place[2]

    def empty(xs, carry):
        out_ref[xs, :HEAD, :] = jnp.zeros((HEAD, QROWS), jnp.bfloat16)
        rows = lax.broadcasted_iota(jnp.int32, (PART - HEAD, QROWS), 0)
        out_ref[xs, HEAD:, :] = jnp.where(rows == 0, FLOOR, 0.0).astype(jnp.bfloat16)
        return carry

    lax.fori_loop(0, x, empty, 0)

    def slab(xs, carry):
        p0 = (xs * (NY * NC) + y * NC + c) * TOK
        last = p0 + TOK - 1
        lane = lax.broadcasted_iota(jnp.int32, (1, QROWS), 1)
        pos = p0 + jnp.where(lane >= TOK, lane - TOK, lane)
        start = jnp.zeros((1, QROWS), jnp.int32)
        first_start = jnp.int32(0)
        last_start = jnp.int32(0)
        end = jnp.int32(0)
        for k in range(DOCS):
            end = end + lengths[k]
            start = jnp.where(pos >= end, end, start)
            first_start = jnp.where(p0 >= end, end, first_start)
            last_start = jnp.where(last >= end, end, last_start)
        q_s[:TOK, :] = q_ref[xs, :, :HEAD]
        q_s[TOK:, :] = q_ref[xs, :, HEAD:]
        m_s[...] = jnp.full((1, QROWS), FLOOR, jnp.float32)
        l_s[...] = jnp.zeros((1, QROWS), jnp.float32)
        acc_s[...] = jnp.zeros((HEAD, QROWS), jnp.float32)

        for ref, core in ((own_ref, c), (peer_ref, 1 - c)):

            def chunk(ch, carry, ref=ref, core=core):
                low = ((x * NY + ch * CHUNK_SLABS) * NC + core) * TOK
                high = low + (CHUNK_SLABS - 1) * NC * TOK + TOK - 1
                rows = pl.ds(pl.multiple_of(ch * CHUNK, CHUNK), CHUNK)

                def update(masked):
                    s = lax.dot_general(
                        ref[rows, :HEAD], q_s[...], NT, preferred_element_type=jnp.float32
                    )
                    s = s * SCALE2
                    if masked:
                        at = lax.broadcasted_iota(jnp.int32, (CHUNK, 1), 0)
                        slab_at = jnp.zeros((CHUNK, 1), jnp.int32)
                        for n in range(1, CHUNK_SLABS):
                            slab_at += (at >= n * TOK).astype(jnp.int32)
                        key_pos = low + at + slab_at * ((NC - 1) * TOK)
                        s = jnp.where((key_pos >= start) & (key_pos <= pos), s, NEG)
                    m_old = m_s[...]
                    m_new = jnp.maximum(m_old, round_up(jnp.max(s, axis=0, keepdims=True)))
                    w = jnp.exp2(s - m_new)
                    fix = jnp.exp2(m_old - m_new)
                    m_s[...] = m_new
                    l_s[...] = l_s[...] * fix + jnp.sum(w, axis=0, keepdims=True)
                    acc_s[...] = acc_s[...] * fix + lax.dot_general(
                        ref[rows, HEAD:],
                        w.astype(jnp.bfloat16),
                        TN,
                        preferred_element_type=jnp.float32,
                    )

                needed = (low <= last) & (high >= first_start)
                whole = (high <= p0) & (low >= last_start)

                @pl.when(needed & whole)
                def _():
                    update(False)

                @pl.when(needed & jnp.logical_not(whole))
                def _():
                    update(True)

                return carry

            lax.fori_loop(0, NY // CHUNK_SLABS, chunk, 0)

        out_ref[xs, :HEAD, :] = acc_s[...].astype(jnp.bfloat16)
        total = l_s[...]
        high_part = total.astype(jnp.bfloat16).astype(jnp.float32)
        rows = lax.broadcasted_iota(jnp.int32, (PART - HEAD, QROWS), 0)
        stats = jnp.where(rows == 0, m_s[...], jnp.where(rows == 1, high_part, total - high_part))
        out_ref[xs, HEAD:, :] = stats.astype(jnp.bfloat16)
        return carry

    lax.fori_loop(x, NX, slab, 0)


def merge_kernel(part_ref, row_ref, col_ref, out_ref):
    m = [part_ref[i, HEAD : HEAD + 1, :].astype(jnp.float32) for i in range(NX)]
    top = jnp.maximum(jnp.maximum(m[0], m[1]), jnp.maximum(m[2], m[3]))
    total = jnp.zeros((1, QROWS), jnp.float32)
    mixed = jnp.zeros((HEAD, QROWS), jnp.float32)
    for i in range(NX):
        w = jnp.exp2(m[i] - top)
        part = part_ref[i, HEAD + 1 : HEAD + 2, :].astype(jnp.float32)
        part = part + part_ref[i, HEAD + 2 : HEAD + 3, :].astype(jnp.float32)
        total = total + w * part
        mixed = mixed + w * part_ref[i, :HEAD, :].astype(jnp.float32)
    attention = (mixed / total).astype(jnp.bfloat16)
    target = row_ref[...]
    earlier = lax.broadcasted_iota(jnp.int32, (TOK, TOK), 0) < lax.broadcasted_iota(
        jnp.int32, (TOK, TOK), 1
    )
    same = (col_ref[...] == target) & earlier
    rank = jnp.sum(same.astype(jnp.int32), axis=0, keepdims=True)
    slot = target * SLOTS + rank
    ids = lax.broadcasted_iota(jnp.int32, (SLOT_TOTAL, TOK), 0)
    placement = (ids == slot).astype(jnp.float32).astype(jnp.bfloat16)
    for h in range(HEADS_HERE):
        out_ref[:, h * HEAD : (h + 1) * HEAD] = lax.dot_general(
            placement,
            attention[:, h * TOK : (h + 1) * TOK],
            NT,
            preferred_element_type=jnp.float32,
        ).astype(jnp.bfloat16)


def collect_kernel(me, owner_ref, in_ref, out_ref):
    mine = (owner_ref[...] == me[0]).astype(jnp.float32).astype(jnp.bfloat16)
    count = lax.dot_general(
        jnp.ones((8, TOK), jnp.bfloat16), mine, NT, preferred_element_type=jnp.float32
    ).astype(jnp.bfloat16)
    before = lax.broadcasted_iota(jnp.int32, (N_DC, N_DC), 0) < lax.broadcasted_iota(
        jnp.int32, (N_DC, N_DC), 1
    )
    first = jnp.dot(
        count, before.astype(jnp.float32).astype(jnp.bfloat16), preferred_element_type=jnp.float32
    ).astype(jnp.bfloat16)
    src = lax.broadcasted_iota(jnp.int32, (N_DC, SLOT_TOTAL), 0)
    slot = lax.broadcasted_iota(jnp.int32, (N_DC, SLOT_TOTAL), 1)
    inside = (slot >= src * SLOTS) & (slot < (src + 1) * SLOTS)
    spread = inside.astype(jnp.float32).astype(jnp.bfloat16)
    count = jnp.dot(count, spread, preferred_element_type=jnp.float32)[:1]
    first = jnp.dot(first, spread, preferred_element_type=jnp.float32)[:1]
    k = (slot[:1] % SLOTS).astype(jnp.float32)
    g = jnp.where(k < count, first + k, -1.0).astype(jnp.int32)
    at = lax.broadcasted_iota(jnp.int32, (TOK, 1), 0)
    part = (at >= 64).astype(jnp.int32) + (at >= 128).astype(jnp.int32)
    within = at - 64 * part
    wanted = ((within // 16) * NJ + part) * 16 + within % 16
    chooser = (g == wanted).astype(jnp.float32).astype(jnp.bfloat16)
    out_ref[...] = jnp.dot(chooser, in_ref[...], preferred_element_type=jnp.float32).astype(
        jnp.bfloat16
    )


def project_kernel(place, x_ref, w0, a1, a2, b1, b2, out_ref):
    c, j = place[0], place[1]
    total = jnp.dot(x_ref[j], w0[...], preferred_element_type=jnp.float32)
    for step, near, far in ((1, a1, b1), (2, a2, b2)):
        rows = x_ref[lax.rem(j + NJ - step, NJ)]
        left, right = rows[:, :HEAD], rows[:, HEAD:]
        lo = jnp.where(c == 0, left, right)
        hi = jnp.where(c == 0, right, left)
        total += jnp.dot(lo, near[...], preferred_element_type=jnp.float32)
        total += jnp.dot(hi, far[...], preferred_element_type=jnp.float32)
    rows = TOK // NJ // NQ
    for n in range(NQ):
        out_ref[n] = total[n * rows : (n + 1) * rows].astype(jnp.bfloat16)


def vmem():
    return pl.BlockSpec(memory_space=pltpu.VMEM)


def near_core(array):
    return pltpu.with_memory_space_constraint(array, pltpu.VMEM)


def far_off(array):
    return pltpu.with_memory_space_constraint(array, pltpu.HBM)


def out_here(*shape):
    return pltpu.VMEM(shape, jnp.bfloat16)


def smem():
    return pl.BlockSpec(memory_space=pltpu.SMEM)


def per_device(queries, keys, values, lengths, mlp_owner, out_weight, residual):
    x, y, c = lax.axis_index("x"), lax.axis_index("y"), lax.axis_index("c")
    j = lax.axis_index("j")
    tp = lax.axis_index("q") * NJ + j
    dc = (x * NY + y) * NC + c
    place = jnp.stack([x, y, c]).astype(jnp.int32)
    peer = [(0, 1), (1, 0)]

    kv_at = tp * HEADS_HERE // GROUP * HEAD
    kv = jnp.concatenate(
        [
            lax.dynamic_slice_in_dim(keys, kv_at, HEAD, 1),
            lax.dynamic_slice_in_dim(values, kv_at, HEAD, 1),
        ],
        axis=1,
    )
    copies = jnp.broadcast_to(queries[None], (NX, TOK, COLS))
    q_all = lax.all_to_all(copies, "x", 0, 0, tiled=True)
    own = lax.all_gather(kv, "y", axis=0, tiled=True)
    other = lax.ppermute(own, "c", peer)
    half = lax.dynamic_slice_in_dim(out_weight, c * HEAD, HEAD, 0)
    half, _ = lax.optimization_barrier((half, own))
    near = [lax.ppermute(half, "j", [(i, (i + s) % NJ) for i in range(NJ)]) for s in (1, 2)]

    partial = pl.pallas_call(
        attend_kernel,
        out_shape=out_here(NX, PART, QROWS),
        in_specs=[smem(), smem(), vmem(), vmem(), vmem()],
        out_specs=vmem(),
        scratch_shapes=[
            pltpu.VMEM((QROWS, HEAD), jnp.bfloat16),
            pltpu.VMEM((1, QROWS), jnp.float32),
            pltpu.VMEM((1, QROWS), jnp.float32),
            pltpu.VMEM((HEAD, QROWS), jnp.float32),
        ],
        name="attend",
    )(place, lengths, near_core(q_all), near_core(own), near_core(other))
    parts = lax.all_to_all(partial, "x", 0, 0, tiled=True)

    targets = lax.dynamic_slice_in_dim(mlp_owner, dc * TOK, TOK, 0)
    outgoing = pl.pallas_call(
        merge_kernel,
        out_shape=out_here(SLOT_TOTAL, COLS),
        in_specs=[vmem(), vmem(), vmem()],
        out_specs=vmem(),
        name="merge",
    )(near_core(parts), targets.reshape(1, TOK), targets.reshape(TOK, 1))
    near, _ = lax.optimization_barrier((near, outgoing))
    far = [lax.ppermute(w, "c", peer) for w in near]
    incoming = lax.all_to_all(
        outgoing.reshape(N_DC, SLOTS, COLS), ("x", "y", "c"), 0, 0, tiled=True
    )
    owned = pl.pallas_call(
        collect_kernel,
        out_shape=out_here(TOK, COLS),
        in_specs=[smem(), vmem(), vmem()],
        out_specs=vmem(),
        name="collect",
    )(
        dc.reshape(1).astype(jnp.int32),
        mlp_owner.reshape(N_DC, TOK),
        near_core(incoming.reshape(SLOT_TOTAL, COLS)),
    )
    shared = lax.all_to_all(owned.reshape(NJ, TOK // NJ, COLS), "j", 0, 0, tiled=True)

    width = out_weight.shape[1]
    rows = TOK // NJ
    tile = 1024
    projected = pl.pallas_call(
        project_kernel,
        out_shape=jax.ShapeDtypeStruct((NQ, rows // NQ, width), jnp.bfloat16),
        grid=(width // tile,),
        in_specs=[smem(), vmem(), pl.BlockSpec((COLS, tile), lambda n: (0, n))]
        + [pl.BlockSpec((HEAD, tile), lambda n: (0, n))] * 4,
        out_specs=pl.BlockSpec((NQ, rows // NQ, tile), lambda n: (0, 0, n)),
        name="project",
    )(jnp.stack([c, j]).astype(jnp.int32), near_core(shared), out_weight, *map(far_off, (*near, *far)))
    q = lax.axis_index("q")
    total = lax.dynamic_index_in_dim(projected, q, 0, keepdims=False).astype(jnp.float32)
    for s in (2, 1, 3):
        block = lax.dynamic_index_in_dim(projected, (q + s) % NQ, 0, keepdims=False)
        moved = lax.ppermute(block, "q", [(i, (i + s) % NQ) for i in range(NQ)])
        total += moved.astype(jnp.float32)
    return (total + residual.astype(jnp.float32)).astype(jnp.bfloat16)


def solution(mesh):
    fine = Mesh(mesh.devices.reshape(NX, NY, NC, NQ, NJ), ("x", "y", "c", "q", "j"))
    dcs, tps = ("x", "y", "c"), ("q", "j")
    return jax.shard_map(
        per_device,
        mesh=fine,
        in_specs=(
            P(dcs, tps),
            P(dcs, None),
            P(dcs, None),
            P(),
            P(),
            P(tps, None),
            P(dcs + tps, None),
        ),
        out_specs=P(dcs + tps, None),
        check_vma=False,
    )
```

```python
import jax
import jax.numpy as jnp
from jax import lax
from jax.experimental import pallas as pl
from jax.experimental.pallas import tpu as pltpu
from jax.sharding import Mesh, PartitionSpec as P

HEAD = 128
GROUP = 4
NX, NY, NC, NQ, NJ = 4, 8, 2, 4, 3
TOK = 192
DOCS = 24
HEADS_HERE = 2
COLS = HEADS_HERE * HEAD
QROWS = HEADS_HERE * TOK
SLOTS = 6
PADDED = 8
OUT = TOK // (NQ * NJ)
N_DC = NX * NY * NC
SLOT_TOTAL = N_DC * SLOTS
CHUNK_SLABS = 4
CHUNK = CHUNK_SLABS * TOK
PART = HEAD + 16
LOG2E = 1.4426950408889634
SCALE2 = HEAD**-0.5 * LOG2E
NEG = -1e30
FLOOR = -1e9


NT = (((1,), (1,)), ((), ()))
TN = (((0,), (0,)), ((), ()))


def round_up(v):
    return (v + jnp.abs(v) * 0.0079).astype(jnp.bfloat16).astype(jnp.float32)


def attend_kernel(place, lengths, q_ref, own_ref, peer_ref, out_ref, q_s, m_s, l_s, acc_s):
    x, y, c = place[0], place[1], place[2]

    def empty(xs, carry):
        out_ref[xs, :HEAD, :] = jnp.zeros((HEAD, QROWS), jnp.bfloat16)
        rows = lax.broadcasted_iota(jnp.int32, (PART - HEAD, QROWS), 0)
        out_ref[xs, HEAD:, :] = jnp.where(rows == 0, FLOOR, 0.0).astype(jnp.bfloat16)
        return carry

    lax.fori_loop(0, x, empty, 0)

    def slab(xs, carry):
        p0 = (xs * (NY * NC) + y * NC + c) * TOK
        last = p0 + TOK - 1
        lane = lax.broadcasted_iota(jnp.int32, (1, QROWS), 1)
        pos = p0 + jnp.where(lane >= TOK, lane - TOK, lane)
        start = jnp.zeros((1, QROWS), jnp.int32)
        first_start = jnp.int32(0)
        last_start = jnp.int32(0)
        end = jnp.int32(0)
        for k in range(DOCS):
            end = end + lengths[k]
            start = jnp.where(pos >= end, end, start)
            first_start = jnp.where(p0 >= end, end, first_start)
            last_start = jnp.where(last >= end, end, last_start)
        q_s[:TOK, :] = q_ref[xs, :, :HEAD]
        q_s[TOK:, :] = q_ref[xs, :, HEAD:]
        m_s[...] = jnp.full((1, QROWS), FLOOR, jnp.float32)
        l_s[...] = jnp.zeros((1, QROWS), jnp.float32)
        acc_s[...] = jnp.zeros((HEAD, QROWS), jnp.float32)

        for ref, core in ((own_ref, c), (peer_ref, 1 - c)):

            def chunk(ch, carry, ref=ref, core=core):
                low = ((x * NY + ch * CHUNK_SLABS) * NC + core) * TOK
                high = low + (CHUNK_SLABS - 1) * NC * TOK + TOK - 1
                rows = pl.ds(pl.multiple_of(ch * CHUNK, CHUNK), CHUNK)

                def update(masked):
                    s = lax.dot_general(
                        ref[rows, :HEAD], q_s[...], NT, preferred_element_type=jnp.float32
                    )
                    s = s * SCALE2
                    if masked:
                        at = lax.broadcasted_iota(jnp.int32, (CHUNK, 1), 0)
                        slab_at = jnp.zeros((CHUNK, 1), jnp.int32)
                        for n in range(1, CHUNK_SLABS):
                            slab_at += (at >= n * TOK).astype(jnp.int32)
                        key_pos = low + at + slab_at * ((NC - 1) * TOK)
                        s = jnp.where((key_pos >= start) & (key_pos <= pos), s, NEG)
                    m_old = m_s[...]
                    m_new = jnp.maximum(m_old, round_up(jnp.max(s, axis=0, keepdims=True)))
                    w = jnp.exp2(s - m_new)
                    fix = jnp.exp2(m_old - m_new)
                    m_s[...] = m_new
                    l_s[...] = l_s[...] * fix + jnp.sum(w, axis=0, keepdims=True)
                    acc_s[...] = acc_s[...] * fix + lax.dot_general(
                        ref[rows, HEAD:],
                        w.astype(jnp.bfloat16),
                        TN,
                        preferred_element_type=jnp.float32,
                    )

                needed = (low <= last) & (high >= first_start)
                whole = (high <= p0) & (low >= last_start)

                @pl.when(needed & whole)
                def _():
                    update(False)

                @pl.when(needed & jnp.logical_not(whole))
                def _():
                    update(True)

                return carry

            lax.fori_loop(0, NY // CHUNK_SLABS, chunk, 0)

        out_ref[xs, :HEAD, :] = acc_s[...].astype(jnp.bfloat16)
        total = l_s[...]
        high_part = total.astype(jnp.bfloat16).astype(jnp.float32)
        rows = lax.broadcasted_iota(jnp.int32, (PART - HEAD, QROWS), 0)
        stats = jnp.where(rows == 0, m_s[...], jnp.where(rows == 1, high_part, total - high_part))
        out_ref[xs, HEAD:, :] = stats.astype(jnp.bfloat16)
        return carry

    lax.fori_loop(x, NX, slab, 0)


def place_kernel(row_ref, col_ref, out_ref):
    target = row_ref[...]
    earlier = lax.broadcasted_iota(jnp.int32, (TOK, TOK), 0) < lax.broadcasted_iota(
        jnp.int32, (TOK, TOK), 1
    )
    same = (col_ref[...] == target) & earlier
    rank = jnp.sum(same.astype(jnp.int32), axis=0, keepdims=True)
    slot = target * PADDED + rank
    ids = lax.broadcasted_iota(jnp.int32, (N_DC * PADDED, TOK), 0)
    out_ref[...] = (ids == slot).astype(jnp.float32).astype(jnp.bfloat16)


def merge_kernel(placement, part_ref, out_ref):
    m = [part_ref[i, HEAD : HEAD + 1, :].astype(jnp.float32) for i in range(NX)]
    top = jnp.maximum(jnp.maximum(m[0], m[1]), jnp.maximum(m[2], m[3]))
    total = jnp.zeros((1, QROWS), jnp.float32)
    mixed = jnp.zeros((HEAD, QROWS), jnp.float32)
    for i in range(NX):
        w = jnp.exp2(m[i] - top)
        part = part_ref[i, HEAD + 1 : HEAD + 2, :].astype(jnp.float32)
        part = part + part_ref[i, HEAD + 2 : HEAD + 3, :].astype(jnp.float32)
        total = total + w * part
        mixed = mixed + w * part_ref[i, :HEAD, :].astype(jnp.float32)
    attention = (mixed / total).astype(jnp.bfloat16)
    for h in range(HEADS_HERE):
        rows = lax.dot_general(
            placement[...],
            attention[:, h * TOK : (h + 1) * TOK],
            NT,
            preferred_element_type=jnp.float32,
        )
        rows = rows.reshape(N_DC, PADDED, HEAD)[:, :SLOTS, :]
        out_ref[:, :, h * HEAD : (h + 1) * HEAD] = rows.astype(jnp.bfloat16)


def choose_kernel(me, owner_ref, out_ref):
    mine = (owner_ref[...] == me[0]).astype(jnp.float32).astype(jnp.bfloat16)
    count = lax.dot_general(
        jnp.ones((8, TOK), jnp.bfloat16), mine, NT, preferred_element_type=jnp.float32
    ).astype(jnp.bfloat16)
    before = lax.broadcasted_iota(jnp.int32, (N_DC, N_DC), 0) < lax.broadcasted_iota(
        jnp.int32, (N_DC, N_DC), 1
    )
    first = jnp.dot(
        count, before.astype(jnp.float32).astype(jnp.bfloat16), preferred_element_type=jnp.float32
    ).astype(jnp.bfloat16)
    src = lax.broadcasted_iota(jnp.int32, (N_DC, SLOT_TOTAL), 0)
    slot = lax.broadcasted_iota(jnp.int32, (N_DC, SLOT_TOTAL), 1)
    inside = (slot >= src * SLOTS) & (slot < (src + 1) * SLOTS)
    spread = inside.astype(jnp.float32).astype(jnp.bfloat16)
    count = jnp.dot(count, spread, preferred_element_type=jnp.float32)[:1]
    first = jnp.dot(first, spread, preferred_element_type=jnp.float32)[:1]
    k = (slot[:1] % SLOTS).astype(jnp.float32)
    g = jnp.where(k < count, first + k, -1.0).astype(jnp.int32)
    at = lax.broadcasted_iota(jnp.int32, (TOK, 1), 0)
    part = (at >= 64).astype(jnp.int32) + (at >= 128).astype(jnp.int32)
    within = at - 64 * part
    wanted = ((within // 16) * NJ + part) * 16 + within % 16
    out_ref[...] = (g == wanted).astype(jnp.float32).astype(jnp.bfloat16)


def collect_kernel(chooser, in_ref, out_ref):
    out_ref[...] = jnp.dot(chooser[...], in_ref[...], preferred_element_type=jnp.float32).astype(
        jnp.bfloat16
    )


def project_kernel(place, x_ref, w0, a1, a2, b1, b2, own_ref, next_ref, prev_ref, c1_ref, c2_ref):
    c, j, q = place[0], place[1], place[2]

    def rows_of(member):
        turned = [
            x_ref[member, pl.ds(pl.multiple_of(lax.rem(q + s, NQ) * OUT, OUT), OUT), :]
            for s in range(NQ)
        ]
        return jnp.concatenate(turned, axis=0)

    total = jnp.dot(rows_of(j), w0[...], preferred_element_type=jnp.float32)
    for step, near, far in ((1, a1, b1), (2, a2, b2)):
        rows = rows_of(lax.rem(j + NJ - step, NJ))
        left, right = rows[:, :HEAD], rows[:, HEAD:]
        lo = jnp.where(c == 0, left, right)
        hi = jnp.where(c == 0, right, left)
        total += jnp.dot(lo, near[...], preferred_element_type=jnp.float32)
        total += jnp.dot(hi, far[...], preferred_element_type=jnp.float32)
    own_ref[...] = total[:OUT]
    next_ref[...] = total[OUT : 2 * OUT]
    c1_ref[...] = total[2 * OUT : 2 * OUT + OUT // 2].astype(jnp.bfloat16)
    c2_ref[...] = total[2 * OUT + OUT // 2 : 3 * OUT].astype(jnp.bfloat16)
    prev_ref[...] = total[3 * OUT :]


def vmem():
    return pl.BlockSpec(memory_space=pltpu.VMEM)


def near_core(array):
    return pltpu.with_memory_space_constraint(array, pltpu.VMEM)


def far_off(array):
    return pltpu.with_memory_space_constraint(array, pltpu.HBM)


def out_here(*shape):
    return pltpu.VMEM(shape, jnp.bfloat16)


def smem():
    return pl.BlockSpec(memory_space=pltpu.SMEM)


def kernel(body, shapes, in_specs, **more):
    return pl.pallas_call(body, out_shape=shapes, in_specs=in_specs, out_specs=vmem(), **more)


def per_device(queries, keys, values, lengths, mlp_owner, out_weight, residual):
    x, y, c = lax.axis_index("x"), lax.axis_index("y"), lax.axis_index("c")
    q, j = lax.axis_index("q"), lax.axis_index("j")
    tp = q * NJ + j
    dc = (x * NY + y) * NC + c
    place = jnp.stack([x, y, c]).astype(jnp.int32)
    peer = [(0, 1), (1, 0)]

    def turn(size, step):
        return [(i, (i + step) % size) for i in range(size)]

    kv_at = tp * HEADS_HERE // GROUP * HEAD
    kv = jnp.concatenate(
        [
            lax.dynamic_slice_in_dim(keys, kv_at, HEAD, 1),
            lax.dynamic_slice_in_dim(values, kv_at, HEAD, 1),
        ],
        axis=1,
    )
    copies = jnp.broadcast_to(queries[None], (NX, TOK, COLS))
    q_all = lax.all_to_all(copies, "x", 0, 0, tiled=True)
    own = lax.all_gather(kv, "y", axis=0, tiled=True)
    other = lax.ppermute(own, "c", peer)

    half = lax.dynamic_slice_in_dim(out_weight, c * HEAD, HEAD, 0)
    half, _ = lax.optimization_barrier((half, own))
    near2 = lax.ppermute(half, "j", turn(NJ, 2))

    partial = kernel(
        attend_kernel,
        out_here(NX, PART, QROWS),
        [smem(), smem(), vmem(), vmem(), vmem()],
        scratch_shapes=[
            pltpu.VMEM((QROWS, HEAD), jnp.bfloat16),
            pltpu.VMEM((1, QROWS), jnp.float32),
            pltpu.VMEM((1, QROWS), jnp.float32),
            pltpu.VMEM((HEAD, QROWS), jnp.float32),
        ],
    )(place, lengths, near_core(q_all), near_core(own), near_core(other))
    half, _ = lax.optimization_barrier((half, partial))
    near1 = lax.ppermute(half, "j", turn(NJ, 1))
    parts = lax.all_to_all(partial, "x", 0, 0, tiled=True)

    targets = lax.dynamic_slice_in_dim(mlp_owner, dc * TOK, TOK, 0)
    placement = kernel(place_kernel, out_here(N_DC * PADDED, TOK), [vmem(), vmem()])(
        targets.reshape(1, TOK), targets.reshape(TOK, 1)
    )
    outgoing = kernel(
        merge_kernel, out_here(N_DC, SLOTS, COLS), [vmem(), vmem()]
    )(near_core(placement), near_core(parts))
    incoming = lax.all_to_all(outgoing, ("x", "y", "c"), 0, 0, tiled=True)
    chooser = kernel(choose_kernel, out_here(TOK, SLOT_TOTAL), [smem(), vmem()])(
        dc.reshape(1).astype(jnp.int32), mlp_owner.reshape(N_DC, TOK)
    )
    owned = kernel(collect_kernel, out_here(TOK, COLS), [vmem(), vmem()])(
        near_core(chooser), near_core(incoming.reshape(SLOT_TOTAL, COLS))
    )
    near2, _ = lax.optimization_barrier((near2, outgoing))
    far2 = lax.ppermute(near2, "c", peer)
    near1, _ = lax.optimization_barrier((near1, owned))
    far1 = lax.ppermute(near1, "c", peer)
    shared = lax.all_to_all(owned.reshape(NJ, TOK // NJ, COLS), "j", 0, 0, tiled=True)

    width = out_weight.shape[1]
    tile = 1024
    blocks = [(OUT, jnp.float32)] * 3 + [(OUT // 2, jnp.bfloat16)] * 2
    mine, ahead, behind, c1, c2 = pl.pallas_call(
        project_kernel,
        out_shape=[jax.ShapeDtypeStruct((n, width), t) for n, t in blocks],
        grid=(width // tile,),
        in_specs=[smem(), vmem(), pl.BlockSpec((COLS, tile), lambda n: (0, n))]
        + [pl.BlockSpec((HEAD, tile), lambda n: (0, n))] * 4,
        out_specs=[pl.BlockSpec((n, tile), lambda n: (0, n)) for n, _ in blocks],
        name="project",
    )(
        jnp.stack([c, j, q]).astype(jnp.int32),
        near_core(shared),
        out_weight,
        *map(far_off, (near1, near2, far1, far2)),
    )
    c1 = lax.ppermute(c1, "q", turn(NQ, 1))
    c2 = lax.ppermute(c2, "q", turn(NQ, 3))
    h = OUT // 2
    ahead = jnp.concatenate([ahead[:h] + c1.astype(jnp.float32), ahead[h:]]).astype(jnp.bfloat16)
    behind = jnp.concatenate([behind[:h], behind[h:] + c2.astype(jnp.float32)]).astype(jnp.bfloat16)
    ahead = lax.ppermute(ahead, "q", turn(NQ, 1))
    behind = lax.ppermute(behind, "q", turn(NQ, 3))
    total = mine + ahead.astype(jnp.float32) + behind.astype(jnp.float32)
    return (total + residual.astype(jnp.float32)).astype(jnp.bfloat16)


def solution(mesh):
    fine = Mesh(mesh.devices.reshape(NX, NY, NC, NQ, NJ), ("x", "y", "c", "q", "j"))
    dcs, tps = ("x", "y", "c"), ("q", "j")

    return jax.shard_map(
        per_device,
        mesh=fine,
        in_specs=(
            P(dcs, tps),
            P(dcs, None),
            P(dcs, None),
            P(),
            P(),
            P(tps, None),
            P(dcs + tps, None),
        ),
        out_specs=P(dcs + tps, None),
        check_vma=False,
    )
```

```python
import jax
import jax.numpy as jnp
from jax import lax
from jax.experimental import pallas as pl
from jax.experimental.pallas import tpu as pltpu
from jax.sharding import Mesh, PartitionSpec as P

HEAD = 128
GROUP = 4
NX, NY, NC, NQ, NJ = 4, 8, 2, 4, 3
TOK = 192
DOCS = 24
HEADS_HERE = 2
COLS = HEADS_HERE * HEAD
QROWS = HEADS_HERE * TOK
SLOTS = 6
PADDED = 8
OUT = TOK // (NQ * NJ)
N_DC = NX * NY * NC
SLOT_TOTAL = N_DC * SLOTS
CHUNK_SLABS = 4
CHUNK = CHUNK_SLABS * TOK
PART = HEAD + 16
LOG2E = 1.4426950408889634
SCALE2 = HEAD**-0.5 * LOG2E
NEG = -1e30
FLOOR = -1e9


NT = (((1,), (1,)), ((), ()))
TN = (((0,), (0,)), ((), ()))


def round_up(v):
    return (v + jnp.abs(v) * 0.0079).astype(jnp.bfloat16).astype(jnp.float32)


def attend_kernel(lengths, q_ref, own_ref, peer_ref, out_ref, q_s, m_s, l_s, acc_s):
    x, y, c = (lax.axis_index(a) for a in ("x", "y", "c"))

    def empty(xs, carry):
        out_ref[xs, :HEAD, :] = jnp.zeros((HEAD, QROWS), jnp.bfloat16)
        rows = lax.broadcasted_iota(jnp.int32, (PART - HEAD, QROWS), 0)
        out_ref[xs, HEAD:, :] = jnp.where(rows == 0, FLOOR, 0.0).astype(jnp.bfloat16)
        return carry

    lax.fori_loop(0, x, empty, 0)

    def slab(xs, carry):
        p0 = (xs * (NY * NC) + y * NC + c) * TOK
        last = p0 + TOK - 1
        lane = lax.broadcasted_iota(jnp.int32, (1, QROWS), 1)
        pos = p0 + jnp.where(lane >= TOK, lane - TOK, lane)
        start = jnp.zeros((1, QROWS), jnp.int32)
        first_start = jnp.int32(0)
        last_start = jnp.int32(0)
        end = jnp.int32(0)
        for k in range(DOCS):
            end = end + lengths[k]
            start = jnp.where(pos >= end, end, start)
            first_start = jnp.where(p0 >= end, end, first_start)
            last_start = jnp.where(last >= end, end, last_start)
        q_s[:TOK, :] = q_ref[xs, :, :HEAD]
        q_s[TOK:, :] = q_ref[xs, :, HEAD:]
        m_s[...] = jnp.full((1, QROWS), FLOOR, jnp.float32)
        l_s[...] = jnp.zeros((1, QROWS), jnp.float32)
        acc_s[...] = jnp.zeros((HEAD, QROWS), jnp.float32)

        for ref, core in ((own_ref, c), (peer_ref, 1 - c)):

            def chunk(ch, carry, ref=ref, core=core):
                low = ((x * NY + ch * CHUNK_SLABS) * NC + core) * TOK
                high = low + (CHUNK_SLABS - 1) * NC * TOK + TOK - 1
                rows = pl.ds(pl.multiple_of(ch * CHUNK, CHUNK), CHUNK)

                def update(masked):
                    s = lax.dot_general(
                        ref[rows, :HEAD], q_s[...], NT, preferred_element_type=jnp.float32
                    )
                    s = s * SCALE2
                    if masked:
                        at = lax.broadcasted_iota(jnp.int32, (CHUNK, 1), 0)
                        slab_at = jnp.zeros((CHUNK, 1), jnp.int32)
                        for n in range(1, CHUNK_SLABS):
                            slab_at += (at >= n * TOK).astype(jnp.int32)
                        key_pos = low + at + slab_at * ((NC - 1) * TOK)
                        s = jnp.where((key_pos >= start) & (key_pos <= pos), s, NEG)
                    m_old = m_s[...]
                    m_new = jnp.maximum(m_old, round_up(jnp.max(s, axis=0, keepdims=True)))
                    w = jnp.exp2(s - m_new)
                    fix = jnp.exp2(m_old - m_new)
                    m_s[...] = m_new
                    l_s[...] = l_s[...] * fix + jnp.sum(w, axis=0, keepdims=True)
                    acc_s[...] = acc_s[...] * fix + lax.dot_general(
                        ref[rows, HEAD:],
                        w.astype(jnp.bfloat16),
                        TN,
                        preferred_element_type=jnp.float32,
                    )

                needed = (low <= last) & (high >= first_start)
                whole = (high <= p0) & (low >= last_start)

                @pl.when(needed & whole)
                def _():
                    update(False)

                @pl.when(needed & jnp.logical_not(whole))
                def _():
                    update(True)

                return carry

            lax.fori_loop(0, NY // CHUNK_SLABS, chunk, 0)

        out_ref[xs, :HEAD, :] = acc_s[...].astype(jnp.bfloat16)
        total = l_s[...]
        high_part = total.astype(jnp.bfloat16).astype(jnp.float32)
        rows = lax.broadcasted_iota(jnp.int32, (PART - HEAD, QROWS), 0)
        stats = jnp.where(rows == 0, m_s[...], jnp.where(rows == 1, high_part, total - high_part))
        out_ref[xs, HEAD:, :] = stats.astype(jnp.bfloat16)
        return carry

    lax.fori_loop(x, NX, slab, 0)


def place_kernel(row_ref, col_ref, out_ref):
    target = row_ref[...]
    earlier = lax.broadcasted_iota(jnp.int32, (TOK, TOK), 0) < lax.broadcasted_iota(
        jnp.int32, (TOK, TOK), 1
    )
    same = (col_ref[...] == target) & earlier
    rank = jnp.sum(same.astype(jnp.int32), axis=0, keepdims=True)
    slot = target * PADDED + rank
    ids = lax.broadcasted_iota(jnp.int32, (N_DC * PADDED, TOK), 0)
    out_ref[...] = (ids == slot).astype(jnp.float32).astype(jnp.bfloat16)


def merge_kernel(placement, part_ref, out_ref):
    m = [part_ref[i, HEAD : HEAD + 1, :].astype(jnp.float32) for i in range(NX)]
    top = jnp.maximum(jnp.maximum(m[0], m[1]), jnp.maximum(m[2], m[3]))
    total = jnp.zeros((1, QROWS), jnp.float32)
    mixed = jnp.zeros((HEAD, QROWS), jnp.float32)
    for i in range(NX):
        w = jnp.exp2(m[i] - top)
        part = part_ref[i, HEAD + 1 : HEAD + 2, :].astype(jnp.float32)
        part = part + part_ref[i, HEAD + 2 : HEAD + 3, :].astype(jnp.float32)
        total = total + w * part
        mixed = mixed + w * part_ref[i, :HEAD, :].astype(jnp.float32)
    attention = (mixed / total).astype(jnp.bfloat16)
    for h in range(HEADS_HERE):
        rows = lax.dot_general(
            placement[...],
            attention[:, h * TOK : (h + 1) * TOK],
            NT,
            preferred_element_type=jnp.float32,
        )
        rows = rows.reshape(N_DC, PADDED, HEAD)[:, :SLOTS, :]
        out_ref[:, :, h * HEAD : (h + 1) * HEAD] = rows.astype(jnp.bfloat16)


def choose_kernel(owner_ref, out_ref):
    x, y, c = (lax.axis_index(a) for a in ("x", "y", "c"))
    mine = (owner_ref[...] == (x * NY + y) * NC + c).astype(jnp.float32).astype(jnp.bfloat16)
    count = lax.dot_general(
        jnp.ones((8, TOK), jnp.bfloat16), mine, NT, preferred_element_type=jnp.float32
    ).astype(jnp.bfloat16)
    before = lax.broadcasted_iota(jnp.int32, (N_DC, N_DC), 0) < lax.broadcasted_iota(
        jnp.int32, (N_DC, N_DC), 1
    )
    first = jnp.dot(
        count, before.astype(jnp.float32).astype(jnp.bfloat16), preferred_element_type=jnp.float32
    ).astype(jnp.bfloat16)
    src = lax.broadcasted_iota(jnp.int32, (N_DC, SLOT_TOTAL), 0)
    slot = lax.broadcasted_iota(jnp.int32, (N_DC, SLOT_TOTAL), 1)
    inside = (slot >= src * SLOTS) & (slot < (src + 1) * SLOTS)
    spread = inside.astype(jnp.float32).astype(jnp.bfloat16)
    count = jnp.dot(count, spread, preferred_element_type=jnp.float32)[:1]
    first = jnp.dot(first, spread, preferred_element_type=jnp.float32)[:1]
    k = (slot[:1] % SLOTS).astype(jnp.float32)
    g = jnp.where(k < count, first + k, -1.0).astype(jnp.int32)
    at = lax.broadcasted_iota(jnp.int32, (TOK, 1), 0)
    part = (at >= 64).astype(jnp.int32) + (at >= 128).astype(jnp.int32)
    within = at - 64 * part
    wanted = ((within // 16) * NJ + part) * 16 + within % 16
    out_ref[...] = (g == wanted).astype(jnp.float32).astype(jnp.bfloat16)


def collect_kernel(chooser, in_ref, out_ref):
    out_ref[...] = jnp.dot(chooser[...], in_ref[...], preferred_element_type=jnp.float32).astype(
        jnp.bfloat16
    )


def project_kernel(x_ref, w0, w1, w2, own_ref, *piece_refs):
    c, j, q = (lax.axis_index(a) for a in ("c", "j", "q"))

    def rows_of(member):
        member = lax.rem(member, NJ)
        turned = [
            x_ref[member, pl.ds(pl.multiple_of(lax.rem(q + s, NQ) * OUT, OUT), OUT), :]
            for s in range(NQ)
        ]
        return jnp.concatenate(turned, axis=0)

    total = jnp.dot(rows_of(j), w0[...], preferred_element_type=jnp.float32)
    total += jnp.dot(rows_of(j + 2 - c), w1[...], preferred_element_type=jnp.float32)
    total += jnp.dot(rows_of(j + 1 + c), w2[...], preferred_element_type=jnp.float32)
    own_ref[...] = total[:OUT]
    half = OUT // 2
    for n, ref in enumerate(piece_refs):
        ref[...] = total[OUT + n * half : OUT + (n + 1) * half].astype(ref.dtype)


def fold_kernel(near_ref, near_add, near_rest, far_rest, far_ref, far_add, ahead_ref, behind_ref):
    half = OUT // 2
    ahead_ref[:half] = (near_ref[...] + near_add[...].astype(jnp.float32)).astype(jnp.bfloat16)
    ahead_ref[half:] = near_rest[...]
    behind_ref[:half] = far_rest[...]
    behind_ref[half:] = (far_ref[...] + far_add[...].astype(jnp.float32)).astype(jnp.bfloat16)


def prepare_kernel(head, q_ref, k_ref, v_ref, copies_ref, kv_ref):
    for i in range(NX):
        copies_ref[i] = q_ref[...]
    kv_ref[:, :HEAD] = k_ref[...]
    kv_ref[:, HEAD:] = v_ref[...]


def vmem():
    return pl.BlockSpec(memory_space=pltpu.VMEM)


def near_core(array):
    return pltpu.with_memory_space_constraint(array, pltpu.VMEM)


def out_here(*shape):
    return pltpu.VMEM(shape, jnp.bfloat16)


def smem():
    return pl.BlockSpec(memory_space=pltpu.SMEM)


def kernel(body, shapes, in_specs, **more):
    outs = [vmem() for _ in shapes] if isinstance(shapes, list) else vmem()
    return pl.pallas_call(body, out_shape=shapes, in_specs=in_specs, out_specs=outs, **more)


def per_device(queries, keys, values, lengths, mlp_owner, out_weight, residual):
    x, y, c = lax.axis_index("x"), lax.axis_index("y"), lax.axis_index("c")
    tp = lax.axis_index("q") * NJ + lax.axis_index("j")
    dc = (x * NY + y) * NC + c
    peer = [(0, 1), (1, 0)]

    def turn(size, step):
        return [(i, (i + step) % size) for i in range(size)]

    around = [
        (k * NJ + i, k * NJ + (i + 1 + k) % NJ) for k in range(NC) for i in range(NJ)
    ]
    turned = lax.ppermute(out_weight, ("c", "j"), around)
    block = pl.BlockSpec((TOK, HEAD), lambda i, head: (0, head[0]))
    copies, kv = pl.pallas_call(
        prepare_kernel,
        out_shape=[
            jax.ShapeDtypeStruct((NX, TOK, COLS), jnp.bfloat16),
            out_here(TOK, COLS),
        ],
        grid_spec=pltpu.PrefetchScalarGridSpec(
            num_scalar_prefetch=1,
            grid=(1,),
            in_specs=[pl.BlockSpec((TOK, COLS), lambda i, head: (0, 0)), block, block],
            out_specs=[
                pl.BlockSpec((NX, TOK, COLS), lambda i, head: (0, 0, 0)),
                pl.BlockSpec((TOK, COLS), lambda i, head: (0, 0)),
            ],
        ),
        name="prepare",
    )((tp * HEADS_HERE // GROUP).reshape(1).astype(jnp.int32), queries, keys, values)
    q_all = lax.all_to_all(copies, "x", 0, 0, tiled=True)
    own = lax.all_gather(kv, "y", axis=0, tiled=True)
    other = lax.ppermute(own, "c", peer)

    partial = kernel(
        attend_kernel,
        out_here(NX, PART, QROWS),
        [smem(), vmem(), vmem(), vmem()],
        scratch_shapes=[
            pltpu.VMEM((QROWS, HEAD), jnp.bfloat16),
            pltpu.VMEM((1, QROWS), jnp.float32),
            pltpu.VMEM((1, QROWS), jnp.float32),
            pltpu.VMEM((HEAD, QROWS), jnp.float32),
        ],
    )(lengths, near_core(q_all), near_core(own), near_core(other))
    parts = lax.all_to_all(partial, "x", 0, 0, tiled=True)

    targets = lax.dynamic_slice_in_dim(mlp_owner, dc * TOK, TOK, 0)
    placement = kernel(place_kernel, out_here(N_DC * PADDED, TOK), [vmem(), vmem()])(
        targets.reshape(1, TOK), targets.reshape(TOK, 1)
    )
    outgoing = kernel(
        merge_kernel, out_here(N_DC, SLOTS, COLS), [vmem(), vmem()]
    )(near_core(placement), near_core(parts))
    incoming = lax.all_to_all(outgoing, ("x", "y", "c"), 0, 0, tiled=True)
    chooser = kernel(choose_kernel, out_here(TOK, SLOT_TOTAL), [vmem()])(
        mlp_owner.reshape(N_DC, TOK)
    )
    owned = kernel(collect_kernel, out_here(TOK, COLS), [vmem(), vmem()])(
        near_core(chooser), near_core(incoming.reshape(SLOT_TOTAL, COLS))
    )
    turned, _ = lax.optimization_barrier((turned, partial))
    swapped = lax.ppermute(turned, "c", peer)
    owned, swapped = lax.optimization_barrier((owned, swapped))
    shared = lax.all_to_all(owned.reshape(NJ, TOK // NJ, COLS), "j", 0, 0, tiled=True)

    width = out_weight.shape[1]
    tile = 1024
    half = OUT // 2
    f32, bf16 = jnp.float32, jnp.bfloat16
    blocks = [(OUT, f32), (half, f32), (half, bf16), (half, bf16), (half, bf16)]
    blocks += [(half, bf16), (half, f32)]
    mine, near, near_rest, c1, c2, far_rest, far = pl.pallas_call(
        project_kernel,
        out_shape=[jax.ShapeDtypeStruct((n, width), t) for n, t in blocks],
        grid=(width // tile,),
        in_specs=[vmem()] + [pl.BlockSpec((COLS, tile), lambda n: (0, n))] * 3,
        out_specs=[pl.BlockSpec((n, tile), lambda n: (0, n)) for n, _ in blocks],
        name="project",
    )(near_core(shared), out_weight, turned, swapped)
    c1 = lax.ppermute(c1, "q", turn(NQ, 1))
    c2 = lax.ppermute(c2, "q", turn(NQ, 3))
    ahead, behind = kernel(fold_kernel, [out_here(OUT, width)] * 2, [vmem()] * 6)(
        near, near_core(c1), near_rest, far_rest, far, near_core(c2)
    )
    ahead = lax.ppermute(ahead, "q", turn(NQ, 1))
    behind = lax.ppermute(behind, "q", turn(NQ, 3))
    total = mine + ahead.astype(jnp.float32) + behind.astype(jnp.float32)
    return (total + residual.astype(jnp.float32)).astype(jnp.bfloat16)


def solution(mesh):
    fine = Mesh(mesh.devices.reshape(NX, NY, NC, NQ, NJ), ("x", "y", "c", "q", "j"))
    dcs, tps = ("x", "y", "c"), ("q", "j")

    return jax.shard_map(
        per_device,
        mesh=fine,
        in_specs=(
            P(dcs, tps),
            P(dcs, None),
            P(dcs, None),
            P(),
            P(),
            P(tps, None),
            P(dcs + tps, None),
        ),
        out_specs=P(dcs + tps, None),
        check_vma=False,
    )
```

```python
import jax
import jax.numpy as jnp
from jax import lax
from jax.experimental import pallas as pl
from jax.experimental.pallas import tpu as pltpu
from jax.sharding import Mesh, PartitionSpec as P

HEAD = 128
GROUP = 4
NX, NY, NC, NQ, NJ = 4, 8, 2, 4, 3
TOK = 192
DOCS = 24
HEADS_HERE = 2
COLS = HEADS_HERE * HEAD
QROWS = HEADS_HERE * TOK
SLOTS = 6
PADDED = 8
OUT = TOK // (NQ * NJ)
N_DC = NX * NY * NC
SLOT_TOTAL = N_DC * SLOTS
CHUNK_SLABS = 4
CHUNK = CHUNK_SLABS * TOK
PART = HEAD + 16
LOG2E = 1.4426950408889634
SCALE2 = HEAD**-0.5 * LOG2E
NEG = -1e30
FLOOR = -1e9


NT = (((1,), (1,)), ((), ()))
TN = (((0,), (0,)), ((), ()))


def round_up(v):
    return (v + jnp.abs(v) * 0.0079).astype(jnp.bfloat16).astype(jnp.float32)


def attend_kernel(lengths, *refs):
    q_refs, (own_ref, peer_ref, out_ref, q_all, q_s, m_s, l_s, acc_s) = refs[:NX], refs[NX:]
    for s, q_ref in enumerate(q_refs):
        q_all[s] = q_ref[...]
    x, y, c = (lax.axis_index(a) for a in ("x", "y", "c"))

    def empty(xs, carry):
        out_ref[xs, :HEAD, :] = jnp.zeros((HEAD, QROWS), jnp.bfloat16)
        rows = lax.broadcasted_iota(jnp.int32, (PART - HEAD, QROWS), 0)
        out_ref[xs, HEAD:, :] = jnp.where(rows == 0, FLOOR, 0.0).astype(jnp.bfloat16)
        return carry

    lax.fori_loop(0, x, empty, 0)

    def slab(xs, carry):
        p0 = (xs * (NY * NC) + y * NC + c) * TOK
        last = p0 + TOK - 1
        lane = lax.broadcasted_iota(jnp.int32, (1, QROWS), 1)
        pos = p0 + jnp.where(lane >= TOK, lane - TOK, lane)
        start = jnp.zeros((1, QROWS), jnp.int32)
        first_start = jnp.int32(0)
        last_start = jnp.int32(0)
        end = jnp.int32(0)
        for k in range(DOCS):
            end = end + lengths[k]
            start = jnp.where(pos >= end, end, start)
            first_start = jnp.where(p0 >= end, end, first_start)
            last_start = jnp.where(last >= end, end, last_start)
        q_s[:TOK, :] = q_all[xs - x, :, :HEAD]
        q_s[TOK:, :] = q_all[xs - x, :, HEAD:]
        m_s[...] = jnp.full((1, QROWS), FLOOR, jnp.float32)
        l_s[...] = jnp.zeros((1, QROWS), jnp.float32)
        acc_s[...] = jnp.zeros((HEAD, QROWS), jnp.float32)

        for ref, core in ((own_ref, c), (peer_ref, 1 - c)):

            def chunk(ch, carry, ref=ref, core=core):
                low = ((x * NY + ch * CHUNK_SLABS) * NC + core) * TOK
                high = low + (CHUNK_SLABS - 1) * NC * TOK + TOK - 1
                rows = pl.ds(pl.multiple_of(ch * CHUNK, CHUNK), CHUNK)

                def update(masked):
                    s = lax.dot_general(
                        ref[rows, :HEAD], q_s[...], NT, preferred_element_type=jnp.float32
                    )
                    s = s * SCALE2
                    if masked:
                        at = lax.broadcasted_iota(jnp.int32, (CHUNK, 1), 0)
                        slab_at = jnp.zeros((CHUNK, 1), jnp.int32)
                        for n in range(1, CHUNK_SLABS):
                            slab_at += (at >= n * TOK).astype(jnp.int32)
                        key_pos = low + at + slab_at * ((NC - 1) * TOK)
                        s = jnp.where((key_pos >= start) & (key_pos <= pos), s, NEG)
                    m_old = m_s[...]
                    m_new = jnp.maximum(m_old, round_up(jnp.max(s, axis=0, keepdims=True)))
                    w = jnp.exp2(s - m_new)
                    fix = jnp.exp2(m_old - m_new)
                    m_s[...] = m_new
                    l_s[...] = l_s[...] * fix + jnp.sum(w, axis=0, keepdims=True)
                    acc_s[...] = acc_s[...] * fix + lax.dot_general(
                        ref[rows, HEAD:],
                        w.astype(jnp.bfloat16),
                        TN,
                        preferred_element_type=jnp.float32,
                    )

                needed = (low <= last) & (high >= first_start)
                whole = (high <= p0) & (low >= last_start)

                @pl.when(needed & whole)
                def _():
                    update(False)

                @pl.when(needed & jnp.logical_not(whole))
                def _():
                    update(True)

                return carry

            lax.fori_loop(0, NY // CHUNK_SLABS, chunk, 0)

        out_ref[xs, :HEAD, :] = acc_s[...].astype(jnp.bfloat16)
        total = l_s[...]
        high_part = total.astype(jnp.bfloat16).astype(jnp.float32)
        rows = lax.broadcasted_iota(jnp.int32, (PART - HEAD, QROWS), 0)
        stats = jnp.where(rows == 0, m_s[...], jnp.where(rows == 1, high_part, total - high_part))
        out_ref[xs, HEAD:, :] = stats.astype(jnp.bfloat16)
        return carry

    lax.fori_loop(x, NX, slab, 0)


def place_kernel(row_ref, col_ref, out_ref):
    target = row_ref[...]
    earlier = lax.broadcasted_iota(jnp.int32, (TOK, TOK), 0) < lax.broadcasted_iota(
        jnp.int32, (TOK, TOK), 1
    )
    same = (col_ref[...] == target) & earlier
    rank = jnp.sum(same.astype(jnp.int32), axis=0, keepdims=True)
    slot = target * PADDED + rank
    ids = lax.broadcasted_iota(jnp.int32, (N_DC * PADDED, TOK), 0)
    out_ref[...] = (ids == slot).astype(jnp.float32).astype(jnp.bfloat16)


def merge_kernel(placement, part_ref, out_ref):
    m = [part_ref[i, HEAD : HEAD + 1, :].astype(jnp.float32) for i in range(NX)]
    top = jnp.maximum(jnp.maximum(m[0], m[1]), jnp.maximum(m[2], m[3]))
    total = jnp.zeros((1, QROWS), jnp.float32)
    mixed = jnp.zeros((HEAD, QROWS), jnp.float32)
    for i in range(NX):
        w = jnp.exp2(m[i] - top)
        part = part_ref[i, HEAD + 1 : HEAD + 2, :].astype(jnp.float32)
        part = part + part_ref[i, HEAD + 2 : HEAD + 3, :].astype(jnp.float32)
        total = total + w * part
        mixed = mixed + w * part_ref[i, :HEAD, :].astype(jnp.float32)
    attention = (mixed / total).astype(jnp.bfloat16)
    for h in range(HEADS_HERE):
        rows = lax.dot_general(
            placement[...],
            attention[:, h * TOK : (h + 1) * TOK],
            NT,
            preferred_element_type=jnp.float32,
        )
        rows = rows.reshape(N_DC, PADDED, HEAD)[:, :SLOTS, :]
        out_ref[:, :, h * HEAD : (h + 1) * HEAD] = rows.astype(jnp.bfloat16)


def choose_kernel(owner_ref, out_ref):
    x, y, c = (lax.axis_index(a) for a in ("x", "y", "c"))
    mine = (owner_ref[...] == (x * NY + y) * NC + c).astype(jnp.float32).astype(jnp.bfloat16)
    count = lax.dot_general(
        jnp.ones((8, TOK), jnp.bfloat16), mine, NT, preferred_element_type=jnp.float32
    ).astype(jnp.bfloat16)
    before = lax.broadcasted_iota(jnp.int32, (N_DC, N_DC), 0) < lax.broadcasted_iota(
        jnp.int32, (N_DC, N_DC), 1
    )
    first = jnp.dot(
        count, before.astype(jnp.float32).astype(jnp.bfloat16), preferred_element_type=jnp.float32
    ).astype(jnp.bfloat16)
    src = lax.broadcasted_iota(jnp.int32, (N_DC, SLOT_TOTAL), 0)
    slot = lax.broadcasted_iota(jnp.int32, (N_DC, SLOT_TOTAL), 1)
    inside = (slot >= src * SLOTS) & (slot < (src + 1) * SLOTS)
    spread = inside.astype(jnp.float32).astype(jnp.bfloat16)
    count = jnp.dot(count, spread, preferred_element_type=jnp.float32)[:1]
    first = jnp.dot(first, spread, preferred_element_type=jnp.float32)[:1]
    k = (slot[:1] % SLOTS).astype(jnp.float32)
    g = jnp.where(k < count, first + k, -1.0).astype(jnp.int32)
    at = lax.broadcasted_iota(jnp.int32, (TOK, 1), 0)
    part = (at >= 64).astype(jnp.int32) + (at >= 128).astype(jnp.int32)
    within = at - 64 * part
    wanted = ((within // 16) * NJ + part) * 16 + within % 16
    out_ref[...] = (g == wanted).astype(jnp.float32).astype(jnp.bfloat16)


def collect_kernel(chooser, in_ref, out_ref):
    out_ref[...] = jnp.dot(chooser[...], in_ref[...], preferred_element_type=jnp.float32).astype(
        jnp.bfloat16
    )


def project_kernel(x_ref, w0, w1, w2, out_ref):
    c, j = lax.axis_index("c"), lax.axis_index("j")
    total = jnp.dot(x_ref[j], w0[...], preferred_element_type=jnp.float32)
    for w, step in ((w1, 2 - c), (w2, 1 + c)):
        rows = x_ref[lax.rem(j + step, NJ)]
        total += jnp.dot(rows, w[...], preferred_element_type=jnp.float32)
    for n in range(NQ):
        out_ref[n] = total[n * OUT : (n + 1) * OUT].astype(jnp.bfloat16)


def prepare_kernel(head, k_ref, v_ref, kv_ref):
    for i in range(NY):
        kv_ref[i, :, :HEAD] = k_ref[...]
        kv_ref[i, :, HEAD:] = v_ref[...]


def vmem():
    return pl.BlockSpec(memory_space=pltpu.VMEM)


def near_core(array):
    return pltpu.with_memory_space_constraint(array, pltpu.VMEM)


def out_here(*shape):
    return pltpu.VMEM(shape, jnp.bfloat16)


def smem():
    return pl.BlockSpec(memory_space=pltpu.SMEM)


def kernel(body, shapes, in_specs, **more):
    outs = [vmem() for _ in shapes] if isinstance(shapes, list) else vmem()
    return pl.pallas_call(body, out_shape=shapes, in_specs=in_specs, out_specs=outs, **more)


def per_device(queries, keys, values, lengths, mlp_owner, out_weight, residual):
    x, y, c = lax.axis_index("x"), lax.axis_index("y"), lax.axis_index("c")
    tp = lax.axis_index("q") * NJ + lax.axis_index("j")
    dc = (x * NY + y) * NC + c
    peer = [(0, 1), (1, 0)]

    around = [
        (k * NJ + i, k * NJ + (i + 1 + k) % NJ) for k in range(NC) for i in range(NJ)
    ]
    turned = lax.ppermute(out_weight, ("c", "j"), around)
    block = pl.BlockSpec((TOK, HEAD), lambda i, head: (0, head[0]))
    kv = pl.pallas_call(
        prepare_kernel,
        out_shape=jax.ShapeDtypeStruct((NY, TOK, COLS), jnp.bfloat16),
        grid_spec=pltpu.PrefetchScalarGridSpec(
            num_scalar_prefetch=1,
            grid=(1,),
            in_specs=[block, block],
            out_specs=pl.BlockSpec((NY, TOK, COLS), lambda i, head: (0, 0, 0)),
        ),
        name="prepare",
    )((tp * HEADS_HERE // GROUP).reshape(1).astype(jnp.int32), keys, values)
    own = lax.all_to_all(kv, "y", 0, 0, tiled=True).reshape(NY * TOK, COLS)
    moved = [lax.ppermute(queries, "x", [(i, i - s) for i in range(s, NX)]) for s in range(1, NX)]
    other = lax.ppermute(own, "c", peer)

    partial = kernel(
        attend_kernel,
        out_here(NX, PART, QROWS),
        [smem()] + [vmem()] * (NX + 2),
        scratch_shapes=[
            pltpu.VMEM((NX, TOK, COLS), jnp.bfloat16),
            pltpu.VMEM((QROWS, HEAD), jnp.bfloat16),
            pltpu.VMEM((1, QROWS), jnp.float32),
            pltpu.VMEM((1, QROWS), jnp.float32),
            pltpu.VMEM((HEAD, QROWS), jnp.float32),
        ],
    )(lengths, queries, *map(near_core, moved), near_core(own), near_core(other))
    parts = lax.all_to_all(partial, "x", 0, 0, tiled=True)

    targets = lax.dynamic_slice_in_dim(mlp_owner, dc * TOK, TOK, 0)
    placement = kernel(place_kernel, out_here(N_DC * PADDED, TOK), [vmem(), vmem()])(
        targets.reshape(1, TOK), targets.reshape(TOK, 1)
    )
    outgoing = kernel(
        merge_kernel, out_here(N_DC, SLOTS, COLS), [vmem(), vmem()]
    )(near_core(placement), near_core(parts))
    incoming = lax.all_to_all(outgoing, ("x", "y", "c"), 0, 0, tiled=True)
    chooser = kernel(choose_kernel, out_here(TOK, SLOT_TOTAL), [vmem()])(
        mlp_owner.reshape(N_DC, TOK)
    )
    owned = kernel(collect_kernel, out_here(TOK, COLS), [vmem(), vmem()])(
        near_core(chooser), near_core(incoming.reshape(SLOT_TOTAL, COLS))
    )
    turned, _ = lax.optimization_barrier((turned, partial))
    swapped = lax.ppermute(turned, "c", peer)
    owned, swapped = lax.optimization_barrier((owned, swapped))
    shared = lax.all_to_all(owned.reshape(NJ, TOK // NJ, COLS), "j", 0, 0, tiled=True)

    width = out_weight.shape[1]
    tile = 1024
    projected = pl.pallas_call(
        project_kernel,
        out_shape=jax.ShapeDtypeStruct((NQ, OUT, width), jnp.bfloat16),
        grid=(width // tile,),
        in_specs=[vmem()] + [pl.BlockSpec((COLS, tile), lambda n: (0, n))] * 3,
        out_specs=pl.BlockSpec((NQ, OUT, tile), lambda n: (0, 0, n)),
        name="project",
    )(near_core(shared), out_weight, turned, swapped)
    blocks = lax.all_to_all(projected, "q", 0, 0, tiled=True)
    total = residual.astype(jnp.float32)
    for n in range(NQ):
        total += blocks[n].astype(jnp.float32)
    return total.astype(jnp.bfloat16)


def solution(mesh):
    fine = Mesh(mesh.devices.reshape(NX, NY, NC, NQ, NJ), ("x", "y", "c", "q", "j"))
    dcs, tps = ("x", "y", "c"), ("q", "j")

    return jax.shard_map(
        per_device,
        mesh=fine,
        in_specs=(
            P(dcs, tps),
            P(dcs, None),
            P(dcs, None),
            P(),
            P(),
            P(tps, None),
            P(dcs + tps, None),
        ),
        out_specs=P(dcs + tps, None),
        check_vma=False,
    )
```

```python
import jax
import jax.numpy as jnp
from jax import lax
from jax.experimental import pallas as pl
from jax.experimental.pallas import tpu as pltpu
from jax.sharding import Mesh, PartitionSpec as P

HEAD = 128
GROUP = 4
NX, NY, NC, NQ, NJ = 4, 8, 2, 4, 3
TOK = 192
DOCS = 24
HEADS_HERE = 2
COLS = HEADS_HERE * HEAD
QROWS = HEADS_HERE * TOK
OUT = TOK // (NQ * NJ)
N_DC = NX * NY * NC
PADDED = 8
SLOT_TOTAL = N_DC * PADDED
CHUNK_SLABS = 4
CHUNK = CHUNK_SLABS * TOK
PART = HEAD + 16
LOG2E = 1.4426950408889634
SCALE2 = HEAD**-0.5 * LOG2E
NEG = -1e30
FLOOR = -1e9


NT = (((1,), (1,)), ((), ()))
TN = (((0,), (0,)), ((), ()))


def round_up(v):
    return (v + jnp.abs(v) * 0.0079).astype(jnp.bfloat16).astype(jnp.float32)


def attend_kernel(lengths, *refs):
    q_refs, (own_ref, peer_ref, out_ref, q_all, q_s, m_s, l_s, acc_s) = refs[:NX], refs[NX:]
    for s, q_ref in enumerate(q_refs):
        q_all[s] = q_ref[...]
    x, y, c = (lax.axis_index(a) for a in ("x", "y", "c"))

    def empty(xs, carry):
        out_ref[xs, :HEAD, :] = jnp.zeros((HEAD, QROWS), jnp.bfloat16)
        rows = lax.broadcasted_iota(jnp.int32, (PART - HEAD, QROWS), 0)
        out_ref[xs, HEAD:, :] = jnp.where(rows == 0, FLOOR, 0.0).astype(jnp.bfloat16)
        return carry

    lax.fori_loop(0, x, empty, 0)

    def slab(xs, carry):
        p0 = (xs * (NY * NC) + y * NC + c) * TOK
        last = p0 + TOK - 1
        lane = lax.broadcasted_iota(jnp.int32, (1, QROWS), 1)
        pos = p0 + jnp.where(lane >= TOK, lane - TOK, lane)
        start = jnp.zeros((1, QROWS), jnp.int32)
        first_start = jnp.int32(0)
        last_start = jnp.int32(0)
        end = jnp.int32(0)
        for k in range(DOCS):
            end = end + lengths[k]
            start = jnp.where(pos >= end, end, start)
            first_start = jnp.where(p0 >= end, end, first_start)
            last_start = jnp.where(last >= end, end, last_start)
        q_s[:TOK, :] = q_all[xs - x, :, :HEAD]
        q_s[TOK:, :] = q_all[xs - x, :, HEAD:]
        m_s[...] = jnp.full((1, QROWS), FLOOR, jnp.float32)
        l_s[...] = jnp.zeros((1, QROWS), jnp.float32)
        acc_s[...] = jnp.zeros((HEAD, QROWS), jnp.float32)

        for ref, core in ((own_ref, c), (peer_ref, 1 - c)):

            def chunk(ch, carry, ref=ref, core=core):
                low = ((x * NY + ch * CHUNK_SLABS) * NC + core) * TOK
                high = low + (CHUNK_SLABS - 1) * NC * TOK + TOK - 1
                rows = pl.ds(pl.multiple_of(ch * CHUNK, CHUNK), CHUNK)

                def update(masked):
                    s = lax.dot_general(
                        ref[rows, :HEAD], q_s[...], NT, preferred_element_type=jnp.float32
                    )
                    s = s * SCALE2
                    if masked:
                        at = lax.broadcasted_iota(jnp.int32, (CHUNK, 1), 0)
                        slab_at = jnp.zeros((CHUNK, 1), jnp.int32)
                        for n in range(1, CHUNK_SLABS):
                            slab_at += (at >= n * TOK).astype(jnp.int32)
                        key_pos = low + at + slab_at * ((NC - 1) * TOK)
                        s = jnp.where((key_pos >= start) & (key_pos <= pos), s, NEG)
                    m_old = m_s[...]
                    m_new = jnp.maximum(m_old, round_up(jnp.max(s, axis=0, keepdims=True)))
                    w = jnp.exp2(s - m_new)
                    fix = jnp.exp2(m_old - m_new)
                    m_s[...] = m_new
                    l_s[...] = l_s[...] * fix + jnp.sum(w, axis=0, keepdims=True)
                    acc_s[...] = acc_s[...] * fix + lax.dot_general(
                        ref[rows, HEAD:],
                        w.astype(jnp.bfloat16),
                        TN,
                        preferred_element_type=jnp.float32,
                    )

                needed = (low <= last) & (high >= first_start)
                whole = (high <= p0) & (low >= last_start)

                @pl.when(needed & whole)
                def _():
                    update(False)

                @pl.when(needed & jnp.logical_not(whole))
                def _():
                    update(True)

                return carry

            lax.fori_loop(0, NY // CHUNK_SLABS, chunk, 0)

        out_ref[xs, :HEAD, :] = acc_s[...].astype(jnp.bfloat16)
        total = l_s[...]
        high_part = total.astype(jnp.bfloat16).astype(jnp.float32)
        rows = lax.broadcasted_iota(jnp.int32, (PART - HEAD, QROWS), 0)
        stats = jnp.where(rows == 0, m_s[...], jnp.where(rows == 1, high_part, total - high_part))
        out_ref[xs, HEAD:, :] = stats.astype(jnp.bfloat16)
        return carry

    lax.fori_loop(x, NX, slab, 0)


def place_kernel(row_ref, col_ref, out_ref):
    target = row_ref[...]
    earlier = lax.broadcasted_iota(jnp.int32, (TOK, TOK), 0) < lax.broadcasted_iota(
        jnp.int32, (TOK, TOK), 1
    )
    same = (col_ref[...] == target) & earlier
    rank = jnp.sum(same.astype(jnp.int32), axis=0, keepdims=True)
    slot = target * PADDED + rank
    ids = lax.broadcasted_iota(jnp.int32, (SLOT_TOTAL, TOK), 0)
    out_ref[...] = (ids == slot).astype(jnp.float32).astype(jnp.bfloat16)


def merge_kernel(placement, part_ref, out_ref):
    m = [part_ref[i, HEAD : HEAD + 1, :].astype(jnp.float32) for i in range(NX)]
    top = jnp.maximum(jnp.maximum(m[0], m[1]), jnp.maximum(m[2], m[3]))
    total = jnp.zeros((1, QROWS), jnp.float32)
    mixed = jnp.zeros((HEAD, QROWS), jnp.float32)
    for i in range(NX):
        w = jnp.exp2(m[i] - top)
        part = part_ref[i, HEAD + 1 : HEAD + 2, :].astype(jnp.float32)
        part = part + part_ref[i, HEAD + 2 : HEAD + 3, :].astype(jnp.float32)
        total = total + w * part
        mixed = mixed + w * part_ref[i, :HEAD, :].astype(jnp.float32)
    attention = (mixed / total).astype(jnp.bfloat16)
    for h in range(HEADS_HERE):
        rows = lax.dot_general(
            placement[...],
            attention[:, h * TOK : (h + 1) * TOK],
            NT,
            preferred_element_type=jnp.float32,
        )
        out_ref[:, h * HEAD : (h + 1) * HEAD] = rows.astype(jnp.bfloat16)


def choose_kernel(owner_ref, out_ref):
    x, y, c = (lax.axis_index(a) for a in ("x", "y", "c"))
    mine = (owner_ref[...] == (x * NY + y) * NC + c).astype(jnp.float32).astype(jnp.bfloat16)
    count = lax.dot_general(
        jnp.ones((8, TOK), jnp.bfloat16), mine, NT, preferred_element_type=jnp.float32
    ).astype(jnp.bfloat16)
    before = lax.broadcasted_iota(jnp.int32, (N_DC, N_DC), 0) < lax.broadcasted_iota(
        jnp.int32, (N_DC, N_DC), 1
    )
    first = jnp.dot(
        count, before.astype(jnp.float32).astype(jnp.bfloat16), preferred_element_type=jnp.float32
    ).astype(jnp.bfloat16)
    src = lax.broadcasted_iota(jnp.int32, (N_DC, SLOT_TOTAL), 0)
    slot = lax.broadcasted_iota(jnp.int32, (N_DC, SLOT_TOTAL), 1)
    inside = (slot >= src * PADDED) & (slot < (src + 1) * PADDED)
    spread = inside.astype(jnp.float32).astype(jnp.bfloat16)
    count = jnp.dot(count, spread, preferred_element_type=jnp.float32)[:1]
    first = jnp.dot(first, spread, preferred_element_type=jnp.float32)[:1]
    k = (slot[:1] % PADDED).astype(jnp.float32)
    g = jnp.where(k < count, first + k, -1.0).astype(jnp.int32)
    at = lax.broadcasted_iota(jnp.int32, (TOK, 1), 0)
    part = (at >= 64).astype(jnp.int32) + (at >= 128).astype(jnp.int32)
    within = at - 64 * part
    wanted = ((within // 16) * NJ + part) * 16 + within % 16
    out_ref[...] = (g == wanted).astype(jnp.float32).astype(jnp.bfloat16)


def collect_kernel(chooser, in_ref, out_ref):
    out_ref[...] = jnp.dot(chooser[...], in_ref[...], preferred_element_type=jnp.float32).astype(
        jnp.bfloat16
    )


def project_kernel(x_ref, w0, w1, w2, out_ref):
    c, j = lax.axis_index("c"), lax.axis_index("j")
    total = jnp.dot(x_ref[j], w0[...], preferred_element_type=jnp.float32)
    total += jnp.dot(x_ref[lax.rem(j + 2 - c, NJ)], w1[...], preferred_element_type=jnp.float32)
    width = w0.shape[1]
    columns = pl.ds(pl.multiple_of(pl.program_id(0) * width, width), width)
    far = x_ref[lax.rem(j + 1 + c, NJ)]
    total += jnp.dot(far, w2[:, columns], preferred_element_type=jnp.float32)
    for n in range(NQ):
        out_ref[n] = total[n * OUT : (n + 1) * OUT].astype(jnp.bfloat16)


def prepare_kernel(head, k_ref, v_ref, kv_ref):
    for i in range(NY):
        kv_ref[i, :, :HEAD] = k_ref[...]
        kv_ref[i, :, HEAD:] = v_ref[...]


def vmem():
    return pl.BlockSpec(memory_space=pltpu.VMEM)


def near_core(array):
    return pltpu.with_memory_space_constraint(array, pltpu.VMEM)


def out_here(*shape):
    return pltpu.VMEM(shape, jnp.bfloat16)


def smem():
    return pl.BlockSpec(memory_space=pltpu.SMEM)


def kernel(body, shapes, in_specs, **more):
    outs = [vmem() for _ in shapes] if isinstance(shapes, list) else vmem()
    return pl.pallas_call(body, out_shape=shapes, in_specs=in_specs, out_specs=outs, **more)


def per_device(queries, keys, values, lengths, mlp_owner, out_weight, residual):
    x, y, c = lax.axis_index("x"), lax.axis_index("y"), lax.axis_index("c")
    tp = lax.axis_index("q") * NJ + lax.axis_index("j")
    dc = (x * NY + y) * NC + c
    peer = [(0, 1), (1, 0)]

    around = [
        (k * NJ + i, k * NJ + (i + 1 + k) % NJ) for k in range(NC) for i in range(NJ)
    ]
    turned = lax.ppermute(out_weight, ("c", "j"), around)
    block = pl.BlockSpec((TOK, HEAD), lambda i, head: (0, head[0]))
    kv = pl.pallas_call(
        prepare_kernel,
        out_shape=jax.ShapeDtypeStruct((NY, TOK, COLS), jnp.bfloat16),
        grid_spec=pltpu.PrefetchScalarGridSpec(
            num_scalar_prefetch=1,
            grid=(1,),
            in_specs=[block, block],
            out_specs=pl.BlockSpec((NY, TOK, COLS), lambda i, head: (0, 0, 0)),
        ),
        name="prepare",
    )((tp * HEADS_HERE // GROUP).reshape(1).astype(jnp.int32), keys, values)
    own = lax.all_to_all(kv, "y", 0, 0, tiled=True).reshape(NY * TOK, COLS)
    moved = [lax.ppermute(queries, "x", [(i, i - s) for i in range(s, NX)]) for s in range(1, NX)]
    other = lax.ppermute(own, "c", peer)

    partial = kernel(
        attend_kernel,
        out_here(NX, PART, QROWS),
        [smem()] + [vmem()] * (NX + 2),
        scratch_shapes=[
            pltpu.VMEM((NX, TOK, COLS), jnp.bfloat16),
            pltpu.VMEM((QROWS, HEAD), jnp.bfloat16),
            pltpu.VMEM((1, QROWS), jnp.float32),
            pltpu.VMEM((1, QROWS), jnp.float32),
            pltpu.VMEM((HEAD, QROWS), jnp.float32),
        ],
    )(lengths, *map(near_core, (queries, *moved)), near_core(own), near_core(other))
    parts = lax.all_to_all(partial, "x", 0, 0, tiled=True)

    targets = lax.dynamic_slice_in_dim(mlp_owner, dc * TOK, TOK, 0)
    placement = kernel(place_kernel, out_here(SLOT_TOTAL, TOK), [vmem(), vmem()])(
        targets.reshape(1, TOK), targets.reshape(TOK, 1)
    )
    outgoing = kernel(
        merge_kernel, out_here(SLOT_TOTAL, COLS), [vmem(), vmem()]
    )(near_core(placement), near_core(parts))
    outgoing = outgoing.reshape(N_DC, PADDED, COLS)
    incoming = lax.all_to_all(outgoing, ("x", "y", "c"), 0, 0, tiled=True)
    chooser = kernel(choose_kernel, out_here(TOK, SLOT_TOTAL), [vmem()])(
        mlp_owner.reshape(N_DC, TOK)
    )
    owned = kernel(collect_kernel, out_here(TOK, COLS), [vmem(), vmem()])(
        near_core(chooser), near_core(incoming.reshape(SLOT_TOTAL, COLS))
    )
    turned, _ = lax.optimization_barrier((turned, outgoing))
    swapped = lax.ppermute(turned, "c", peer)
    owned, swapped = lax.optimization_barrier((owned, swapped))
    shared = lax.all_to_all(owned.reshape(NJ, TOK // NJ, COLS), "j", 0, 0, tiled=True)

    width = out_weight.shape[1]
    tile = 1024
    projected = pl.pallas_call(
        project_kernel,
        out_shape=jax.ShapeDtypeStruct((NQ, OUT, width), jnp.bfloat16),
        grid=(width // tile,),
        in_specs=[vmem()] + [pl.BlockSpec((COLS, tile), lambda n: (0, n))] * 2 + [vmem()],
        out_specs=pl.BlockSpec((NQ, OUT, tile), lambda n: (0, 0, n)),
        name="project",
    )(near_core(shared), out_weight, turned, near_core(swapped))
    blocks = lax.all_to_all(projected, "q", 0, 0, tiled=True)
    total = residual.astype(jnp.float32)
    for n in range(NQ):
        total += blocks[n].astype(jnp.float32)
    return total.astype(jnp.bfloat16)


def solution(mesh):
    fine = Mesh(mesh.devices.reshape(NX, NY, NC, NQ, NJ), ("x", "y", "c", "q", "j"))
    dcs, tps = ("x", "y", "c"), ("q", "j")

    return jax.shard_map(
        per_device,
        mesh=fine,
        in_specs=(
            P(dcs, tps),
            P(dcs, None),
            P(dcs, None),
            P(),
            P(),
            P(tps, None),
            P(dcs + tps, None),
        ),
        out_specs=P(dcs + tps, None),
        check_vma=False,
    )
```

```python
import jax
import jax.numpy as jnp
from jax import lax
from jax.experimental import pallas as pl
from jax.experimental.pallas import tpu as pltpu
from jax.sharding import Mesh, PartitionSpec as P

HEAD = 128
GROUP = 4
NX, NY, NC, NQ, NJ = 4, 8, 2, 4, 3
TOK = 192
DOCS = 24
HEADS_HERE = 2
COLS = HEADS_HERE * HEAD
QROWS = HEADS_HERE * TOK
OUT = TOK // (NQ * NJ)
N_DC = NX * NY * NC
PADDED = 8
SLOT_TOTAL = N_DC * PADDED
PIECE = TOK // NX
CHUNK = NY * PIECE
PART = HEAD + 16
LOG2E = 1.4426950408889634
SCALE2 = HEAD**-0.5 * LOG2E
NEG = -1e30
FLOOR = -1e9


NT = (((1,), (1,)), ((), ()))
TN = (((0,), (0,)), ((), ()))


def round_up(v):
    return (v + jnp.abs(v) * 0.0079).astype(jnp.bfloat16).astype(jnp.float32)


def attend_kernel(lengths, *refs):
    q_refs, (own_ref, peer_ref, out_ref, q_all, q_s, m_s, l_s, acc_s) = refs[:NX], refs[NX:]
    for s, q_ref in enumerate(q_refs):
        q_all[s] = q_ref[...]
    x, y, c = (lax.axis_index(a) for a in ("x", "y", "c"))

    def slab(turn, carry):
        xs = lax.rem(x + turn, NX)
        p0 = (xs * (NY * NC) + y * NC + c) * TOK
        last = p0 + TOK - 1
        lane = lax.broadcasted_iota(jnp.int32, (1, QROWS), 1)
        pos = p0 + jnp.where(lane >= TOK, lane - TOK, lane)
        start = jnp.zeros((1, QROWS), jnp.int32)
        first_start = jnp.int32(0)
        last_start = jnp.int32(0)
        end = jnp.int32(0)
        for k in range(DOCS):
            end = end + lengths[k]
            start = jnp.where(pos >= end, end, start)
            first_start = jnp.where(p0 >= end, end, first_start)
            last_start = jnp.where(last >= end, end, last_start)
        q_s[:TOK, :] = q_all[turn, :, :HEAD]
        q_s[TOK:, :] = q_all[turn, :, HEAD:]
        m_s[...] = jnp.full((1, QROWS), FLOOR, jnp.float32)
        l_s[...] = jnp.zeros((1, QROWS), jnp.float32)
        acc_s[...] = jnp.zeros((HEAD, QROWS), jnp.float32)

        for ref, core in ((own_ref, c), (peer_ref, 1 - c)):

            def chunk(ch, carry, ref=ref, core=core):
                low = (ch * NY * NC + core) * TOK + x * PIECE
                high = low + (NY - 1) * NC * TOK + PIECE - 1
                rows = pl.ds(pl.multiple_of(ch * CHUNK, CHUNK), CHUNK)

                def update(masked):
                    s = lax.dot_general(
                        ref[rows, :HEAD], q_s[...], NT, preferred_element_type=jnp.float32
                    )
                    s = s * SCALE2
                    if masked:
                        at = lax.broadcasted_iota(jnp.int32, (CHUNK, 1), 0)
                        slab_at = jnp.zeros((CHUNK, 1), jnp.int32)
                        for n in range(1, NY):
                            slab_at += (at >= n * PIECE).astype(jnp.int32)
                        key_pos = low + at + slab_at * (NC * TOK - PIECE)
                        s = jnp.where((key_pos >= start) & (key_pos <= pos), s, NEG)
                    m_old = m_s[...]
                    m_new = jnp.maximum(m_old, round_up(jnp.max(s, axis=0, keepdims=True)))
                    w = jnp.exp2(s - m_new)
                    fix = jnp.exp2(m_old - m_new)
                    m_s[...] = m_new
                    l_s[...] = l_s[...] * fix + jnp.sum(w, axis=0, keepdims=True)
                    acc_s[...] = acc_s[...] * fix + lax.dot_general(
                        ref[rows, HEAD:],
                        w.astype(jnp.bfloat16),
                        TN,
                        preferred_element_type=jnp.float32,
                    )

                needed = (low <= last) & (high >= first_start)
                whole = (high <= p0) & (low >= last_start)

                @pl.when(needed & whole)
                def _():
                    update(False)

                @pl.when(needed & jnp.logical_not(whole))
                def _():
                    update(True)

                return carry

            lax.fori_loop(0, NX, chunk, 0)

        out_ref[xs, :HEAD, :] = acc_s[...].astype(jnp.bfloat16)
        total = l_s[...]
        high_part = total.astype(jnp.bfloat16).astype(jnp.float32)
        rows = lax.broadcasted_iota(jnp.int32, (PART - HEAD, QROWS), 0)
        stats = jnp.where(rows == 0, m_s[...], jnp.where(rows == 1, high_part, total - high_part))
        out_ref[xs, HEAD:, :] = stats.astype(jnp.bfloat16)
        return carry

    lax.fori_loop(0, NX, slab, 0)


def place_kernel(row_ref, col_ref, out_ref):
    target = row_ref[...]
    earlier = lax.broadcasted_iota(jnp.int32, (TOK, TOK), 0) < lax.broadcasted_iota(
        jnp.int32, (TOK, TOK), 1
    )
    same = (col_ref[...] == target) & earlier
    rank = jnp.sum(same.astype(jnp.int32), axis=0, keepdims=True)
    slot = target * PADDED + rank
    ids = lax.broadcasted_iota(jnp.int32, (SLOT_TOTAL, TOK), 0)
    out_ref[...] = (ids == slot).astype(jnp.float32).astype(jnp.bfloat16)


def merge_kernel(placement, part_ref, out_ref):
    m = [part_ref[i, HEAD : HEAD + 1, :].astype(jnp.float32) for i in range(NX)]
    top = jnp.maximum(jnp.maximum(m[0], m[1]), jnp.maximum(m[2], m[3]))
    total = jnp.zeros((1, QROWS), jnp.float32)
    mixed = jnp.zeros((HEAD, QROWS), jnp.float32)
    for i in range(NX):
        w = jnp.exp2(m[i] - top)
        part = part_ref[i, HEAD + 1 : HEAD + 2, :].astype(jnp.float32)
        part = part + part_ref[i, HEAD + 2 : HEAD + 3, :].astype(jnp.float32)
        total = total + w * part
        mixed = mixed + w * part_ref[i, :HEAD, :].astype(jnp.float32)
    attention = (mixed / total).astype(jnp.bfloat16)
    for h in range(HEADS_HERE):
        rows = lax.dot_general(
            placement[...],
            attention[:, h * TOK : (h + 1) * TOK],
            NT,
            preferred_element_type=jnp.float32,
        )
        out_ref[:, h * HEAD : (h + 1) * HEAD] = rows.astype(jnp.bfloat16)


def choose_kernel(owner_ref, out_ref):
    x, y, c = (lax.axis_index(a) for a in ("x", "y", "c"))
    mine = (owner_ref[...] == (x * NY + y) * NC + c).astype(jnp.float32).astype(jnp.bfloat16)
    count = lax.dot_general(
        jnp.ones((8, TOK), jnp.bfloat16), mine, NT, preferred_element_type=jnp.float32
    ).astype(jnp.bfloat16)
    before = lax.broadcasted_iota(jnp.int32, (N_DC, N_DC), 0) < lax.broadcasted_iota(
        jnp.int32, (N_DC, N_DC), 1
    )
    first = jnp.dot(
        count, before.astype(jnp.float32).astype(jnp.bfloat16), preferred_element_type=jnp.float32
    ).astype(jnp.bfloat16)
    src = lax.broadcasted_iota(jnp.int32, (N_DC, SLOT_TOTAL), 0)
    slot = lax.broadcasted_iota(jnp.int32, (N_DC, SLOT_TOTAL), 1)
    inside = (slot >= src * PADDED) & (slot < (src + 1) * PADDED)
    spread = inside.astype(jnp.float32).astype(jnp.bfloat16)
    count = jnp.dot(count, spread, preferred_element_type=jnp.float32)[:1]
    first = jnp.dot(first, spread, preferred_element_type=jnp.float32)[:1]
    k = (slot[:1] % PADDED).astype(jnp.float32)
    g = jnp.where(k < count, first + k, -1.0).astype(jnp.int32)
    at = lax.broadcasted_iota(jnp.int32, (TOK, 1), 0)
    part = (at >= 64).astype(jnp.int32) + (at >= 128).astype(jnp.int32)
    within = at - 64 * part
    wanted = ((within // 16) * NJ + part) * 16 + within % 16
    out_ref[...] = (g == wanted).astype(jnp.float32).astype(jnp.bfloat16)


def collect_kernel(chooser, in_ref, out_ref):
    out_ref[...] = jnp.dot(chooser[...], in_ref[...], preferred_element_type=jnp.float32).astype(
        jnp.bfloat16
    )


def project_kernel(x_ref, w0, w1, w2, out_ref):
    c, j = lax.axis_index("c"), lax.axis_index("j")
    total = jnp.dot(x_ref[j], w0[...], preferred_element_type=jnp.float32)
    total += jnp.dot(x_ref[lax.rem(j + 2 - c, NJ)], w1[...], preferred_element_type=jnp.float32)
    width = w0.shape[1]
    columns = pl.ds(pl.multiple_of(pl.program_id(0) * width, width), width)
    far = x_ref[lax.rem(j + 1 + c, NJ)]
    total += jnp.dot(far, w2[:, columns], preferred_element_type=jnp.float32)
    for n in range(NQ):
        out_ref[n] = total[n * OUT : (n + 1) * OUT].astype(jnp.bfloat16)


def prepare_kernel(head, k_ref, v_ref, kv_ref):
    for i in range(NX * NY):
        rows = pl.ds(i // NY * PIECE, PIECE)
        kv_ref[i, :, :HEAD] = k_ref[rows, :]
        kv_ref[i, :, HEAD:] = v_ref[rows, :]


def vmem():
    return pl.BlockSpec(memory_space=pltpu.VMEM)


def near_core(array):
    return pltpu.with_memory_space_constraint(array, pltpu.VMEM)


def out_here(*shape):
    return pltpu.VMEM(shape, jnp.bfloat16)


def smem():
    return pl.BlockSpec(memory_space=pltpu.SMEM)


def kernel(body, shapes, in_specs, **more):
    outs = [vmem() for _ in shapes] if isinstance(shapes, list) else vmem()
    return pl.pallas_call(body, out_shape=shapes, in_specs=in_specs, out_specs=outs, **more)


def per_device(queries, keys, values, lengths, mlp_owner, out_weight, residual):
    x, y, c = lax.axis_index("x"), lax.axis_index("y"), lax.axis_index("c")
    tp = lax.axis_index("q") * NJ + lax.axis_index("j")
    dc = (x * NY + y) * NC + c
    peer = [(0, 1), (1, 0)]

    def turn(size, step):
        return [(i, (i + step) % size) for i in range(size)]

    around = [
        (k * NJ + i, k * NJ + (i + 1 + k) % NJ) for k in range(NC) for i in range(NJ)
    ]
    turned = lax.ppermute(out_weight, ("c", "j"), around)
    block = pl.BlockSpec((TOK, HEAD), lambda i, head: (0, head[0]))
    kv = pl.pallas_call(
        prepare_kernel,
        out_shape=jax.ShapeDtypeStruct((NX * NY, PIECE, COLS), jnp.bfloat16),
        grid_spec=pltpu.PrefetchScalarGridSpec(
            num_scalar_prefetch=1,
            grid=(1,),
            in_specs=[block, block],
            out_specs=pl.BlockSpec((NX * NY, PIECE, COLS), lambda i, head: (0, 0, 0)),
        ),
        name="prepare",
    )((tp * HEADS_HERE // GROUP).reshape(1).astype(jnp.int32), keys, values)
    own = lax.all_to_all(kv, ("x", "y"), 0, 0, tiled=True).reshape(NY * TOK, COLS)
    moved = [
        lax.ppermute(queries, "x", turn(NX, NX - s)) for s in range(1, NX)
    ]
    other = lax.ppermute(own, "c", peer)

    partial = kernel(
        attend_kernel,
        out_here(NX, PART, QROWS),
        [smem()] + [vmem()] * (NX + 2),
        scratch_shapes=[
            pltpu.VMEM((NX, TOK, COLS), jnp.bfloat16),
            pltpu.VMEM((QROWS, HEAD), jnp.bfloat16),
            pltpu.VMEM((1, QROWS), jnp.float32),
            pltpu.VMEM((1, QROWS), jnp.float32),
            pltpu.VMEM((HEAD, QROWS), jnp.float32),
        ],
    )(lengths, *map(near_core, (queries, *moved)), near_core(own), near_core(other))
    parts = lax.all_to_all(partial, "x", 0, 0, tiled=True)

    targets = lax.dynamic_slice_in_dim(mlp_owner, dc * TOK, TOK, 0)
    placement = kernel(place_kernel, out_here(SLOT_TOTAL, TOK), [vmem(), vmem()])(
        targets.reshape(1, TOK), targets.reshape(TOK, 1)
    )
    outgoing = kernel(
        merge_kernel, out_here(SLOT_TOTAL, COLS), [vmem(), vmem()]
    )(near_core(placement), near_core(parts))
    outgoing = outgoing.reshape(N_DC, PADDED, COLS)
    incoming = lax.all_to_all(outgoing, ("x", "y", "c"), 0, 0, tiled=True)
    chooser = kernel(choose_kernel, out_here(TOK, SLOT_TOTAL), [vmem()])(
        mlp_owner.reshape(N_DC, TOK)
    )
    owned = kernel(collect_kernel, out_here(TOK, COLS), [vmem(), vmem()])(
        near_core(chooser), near_core(incoming.reshape(SLOT_TOTAL, COLS))
    )
    turned, _ = lax.optimization_barrier((turned, outgoing))
    swapped = lax.ppermute(turned, "c", peer)
    owned, swapped = lax.optimization_barrier((owned, swapped))
    shared = lax.all_to_all(owned.reshape(NJ, TOK // NJ, COLS), "j", 0, 0, tiled=True)

    width = out_weight.shape[1]
    tile = 1024
    projected = pl.pallas_call(
        project_kernel,
        out_shape=jax.ShapeDtypeStruct((NQ, OUT, width), jnp.bfloat16),
        grid=(width // tile,),
        in_specs=[vmem()] + [pl.BlockSpec((COLS, tile), lambda n: (0, n))] * 2 + [vmem()],
        out_specs=pl.BlockSpec((NQ, OUT, tile), lambda n: (0, 0, n)),
        name="project",
    )(near_core(shared), out_weight, turned, near_core(swapped))
    blocks = lax.all_to_all(projected, "q", 0, 0, tiled=True)
    total = residual.astype(jnp.float32)
    for n in range(NQ):
        total += blocks[n].astype(jnp.float32)
    return total.astype(jnp.bfloat16)


def solution(mesh):
    fine = Mesh(mesh.devices.reshape(NX, NY, NC, NQ, NJ), ("x", "y", "c", "q", "j"))
    dcs, tps = ("x", "y", "c"), ("q", "j")

    return jax.shard_map(
        per_device,
        mesh=fine,
        in_specs=(
            P(dcs, tps),
            P(dcs, None),
            P(dcs, None),
            P(),
            P(),
            P(tps, None),
            P(dcs + tps, None),
        ),
        out_specs=P(dcs + tps, None),
        check_vma=False,
    )
```

```python
import jax
import jax.numpy as jnp
from jax import lax
from jax.experimental import pallas as pl
from jax.experimental.pallas import tpu as pltpu
from jax.sharding import Mesh, PartitionSpec as P

HEAD = 128
GROUP = 4
NX, NY, NC, NQ, NJ = 4, 8, 2, 4, 3
TOK = 192
DOCS = 24
HEADS_HERE = 2
COLS = HEADS_HERE * HEAD
QROWS = HEADS_HERE * TOK
OUT = TOK // (NQ * NJ)
N_DC = NX * NY * NC
PADDED = 8
SLOT_TOTAL = N_DC * PADDED
CHUNK_SLABS = 4
CHUNK = CHUNK_SLABS * TOK
PART = HEAD + 16
LOG2E = 1.4426950408889634
SCALE2 = HEAD**-0.5 * LOG2E
NEG = -1e30
FLOOR = -1e9


NT = (((1,), (1,)), ((), ()))
TN = (((0,), (0,)), ((), ()))


def round_up(v):
    return (v + jnp.abs(v) * 0.0079).astype(jnp.bfloat16).astype(jnp.float32)


def attend_kernel(lengths, *refs):
    q_refs, (own_ref, peer_ref, out_ref, q_all, q_s, m_s, l_s, acc_s) = refs[:NX], refs[NX:]
    for s, q_ref in enumerate(q_refs):
        q_all[s] = q_ref[...]
    x, y, c = (lax.axis_index(a) for a in ("x", "y", "c"))

    def empty(xs, carry):
        out_ref[xs, :HEAD, :] = jnp.zeros((HEAD, QROWS), jnp.bfloat16)
        rows = lax.broadcasted_iota(jnp.int32, (PART - HEAD, QROWS), 0)
        out_ref[xs, HEAD:, :] = jnp.where(rows == 0, FLOOR, 0.0).astype(jnp.bfloat16)
        return carry

    lax.fori_loop(0, x, empty, 0)

    def slab(xs, carry):
        p0 = (xs * (NY * NC) + y * NC + c) * TOK
        last = p0 + TOK - 1
        lane = lax.broadcasted_iota(jnp.int32, (1, QROWS), 1)
        pos = p0 + jnp.where(lane >= TOK, lane - TOK, lane)
        start = jnp.zeros((1, QROWS), jnp.int32)
        first_start = jnp.int32(0)
        last_start = jnp.int32(0)
        end = jnp.int32(0)
        for k in range(DOCS):
            end = end + lengths[k]
            start = jnp.where(pos >= end, end, start)
            first_start = jnp.where(p0 >= end, end, first_start)
            last_start = jnp.where(last >= end, end, last_start)
        q_s[:TOK, :] = q_all[xs - x, :, :HEAD]
        q_s[TOK:, :] = q_all[xs - x, :, HEAD:]
        m_s[...] = jnp.full((1, QROWS), FLOOR, jnp.float32)
        l_s[...] = jnp.zeros((1, QROWS), jnp.float32)
        acc_s[...] = jnp.zeros((HEAD, QROWS), jnp.float32)

        def chunk(ch, carry):
            low = (x * NY + ch * CHUNK_SLABS) * NC * TOK
            high = low + CHUNK_SLABS * NC * TOK - 1
            rows = pl.ds(pl.multiple_of(ch * CHUNK, CHUNK), CHUNK)

            def update(masked):
                pieces = []
                for ref, core in ((own_ref, c), (peer_ref, 1 - c)):
                    s = lax.dot_general(
                        ref[rows, :HEAD], q_s[...], NT, preferred_element_type=jnp.float32
                    )
                    s = s * SCALE2
                    if masked:
                        at = lax.broadcasted_iota(jnp.int32, (CHUNK, 1), 0)
                        slab_at = jnp.zeros((CHUNK, 1), jnp.int32)
                        for n in range(1, CHUNK_SLABS):
                            slab_at += (at >= n * TOK).astype(jnp.int32)
                        key_pos = low + core * TOK + at + slab_at * ((NC - 1) * TOK)
                        s = jnp.where((key_pos >= start) & (key_pos <= pos), s, NEG)
                    pieces.append(s)
                m_old = m_s[...]
                top = [jnp.max(s, axis=0, keepdims=True) for s in pieces]
                m_new = jnp.maximum(m_old, round_up(jnp.maximum(top[0], top[1])))
                fix = jnp.exp2(m_old - m_new)
                m_s[...] = m_new
                total = l_s[...] * fix
                mixed = acc_s[...] * fix
                for s, ref in zip(pieces, (own_ref, peer_ref)):
                    w = jnp.exp2(s - m_new)
                    total = total + jnp.sum(w, axis=0, keepdims=True)
                    mixed = mixed + lax.dot_general(
                        ref[rows, HEAD:],
                        w.astype(jnp.bfloat16),
                        TN,
                        preferred_element_type=jnp.float32,
                    )
                l_s[...] = total
                acc_s[...] = mixed

            needed = (low <= last) & (high >= first_start)
            whole = (high <= p0) & (low >= last_start)

            @pl.when(needed & whole)
            def _():
                update(False)

            @pl.when(needed & jnp.logical_not(whole))
            def _():
                update(True)

            return carry

        lax.fori_loop(0, NY // CHUNK_SLABS, chunk, 0)

        out_ref[xs, :HEAD, :] = acc_s[...].astype(jnp.bfloat16)
        total = l_s[...]
        high_part = total.astype(jnp.bfloat16).astype(jnp.float32)
        rows = lax.broadcasted_iota(jnp.int32, (PART - HEAD, QROWS), 0)
        stats = jnp.where(rows == 0, m_s[...], jnp.where(rows == 1, high_part, total - high_part))
        out_ref[xs, HEAD:, :] = stats.astype(jnp.bfloat16)
        return carry

    lax.fori_loop(x, NX, slab, 0)


def place_kernel(row_ref, col_ref, out_ref):
    target = row_ref[...]
    earlier = lax.broadcasted_iota(jnp.int32, (TOK, TOK), 0) < lax.broadcasted_iota(
        jnp.int32, (TOK, TOK), 1
    )
    same = (col_ref[...] == target) & earlier
    rank = jnp.sum(same.astype(jnp.int32), axis=0, keepdims=True)
    slot = target * PADDED + rank
    ids = lax.broadcasted_iota(jnp.int32, (SLOT_TOTAL, TOK), 0)
    out_ref[...] = (ids == slot).astype(jnp.float32).astype(jnp.bfloat16)


def merge_kernel(placement, part_ref, out_ref):
    m = [part_ref[i, HEAD : HEAD + 1, :].astype(jnp.float32) for i in range(NX)]
    top = jnp.maximum(jnp.maximum(m[0], m[1]), jnp.maximum(m[2], m[3]))
    total = jnp.zeros((1, QROWS), jnp.float32)
    mixed = jnp.zeros((HEAD, QROWS), jnp.float32)
    for i in range(NX):
        w = jnp.exp2(m[i] - top)
        part = part_ref[i, HEAD + 1 : HEAD + 2, :].astype(jnp.float32)
        part = part + part_ref[i, HEAD + 2 : HEAD + 3, :].astype(jnp.float32)
        total = total + w * part
        mixed = mixed + w * part_ref[i, :HEAD, :].astype(jnp.float32)
    attention = (mixed / total).astype(jnp.bfloat16)
    for h in range(HEADS_HERE):
        rows = lax.dot_general(
            placement[...],
            attention[:, h * TOK : (h + 1) * TOK],
            NT,
            preferred_element_type=jnp.float32,
        )
        out_ref[:, h * HEAD : (h + 1) * HEAD] = rows.astype(jnp.bfloat16)


def choose_kernel(owner_ref, out_ref):
    x, y, c = (lax.axis_index(a) for a in ("x", "y", "c"))
    mine = (owner_ref[...] == (x * NY + y) * NC + c).astype(jnp.float32).astype(jnp.bfloat16)
    count = lax.dot_general(
        jnp.ones((8, TOK), jnp.bfloat16), mine, NT, preferred_element_type=jnp.float32
    ).astype(jnp.bfloat16)
    before = lax.broadcasted_iota(jnp.int32, (N_DC, N_DC), 0) < lax.broadcasted_iota(
        jnp.int32, (N_DC, N_DC), 1
    )
    first = jnp.dot(
        count, before.astype(jnp.float32).astype(jnp.bfloat16), preferred_element_type=jnp.float32
    ).astype(jnp.bfloat16)
    src = lax.broadcasted_iota(jnp.int32, (N_DC, SLOT_TOTAL), 0)
    slot = lax.broadcasted_iota(jnp.int32, (N_DC, SLOT_TOTAL), 1)
    inside = (slot >= src * PADDED) & (slot < (src + 1) * PADDED)
    spread = inside.astype(jnp.float32).astype(jnp.bfloat16)
    count = jnp.dot(count, spread, preferred_element_type=jnp.float32)[:1]
    first = jnp.dot(first, spread, preferred_element_type=jnp.float32)[:1]
    k = (slot[:1] % PADDED).astype(jnp.float32)
    g = jnp.where(k < count, first + k, -1.0).astype(jnp.int32)
    at = lax.broadcasted_iota(jnp.int32, (TOK, 1), 0)
    part = (at >= 64).astype(jnp.int32) + (at >= 128).astype(jnp.int32)
    within = at - 64 * part
    wanted = ((within // 16) * NJ + part) * 16 + within % 16
    out_ref[...] = (g == wanted).astype(jnp.float32).astype(jnp.bfloat16)


def collect_kernel(chooser, in_ref, out_ref):
    out_ref[...] = jnp.dot(chooser[...], in_ref[...], preferred_element_type=jnp.float32).astype(
        jnp.bfloat16
    )


def project_kernel(x_ref, w0, w1, w2, out_ref):
    c, j = lax.axis_index("c"), lax.axis_index("j")
    total = jnp.dot(x_ref[j], w0[...], preferred_element_type=jnp.float32)
    total += jnp.dot(x_ref[lax.rem(j + 2 - c, NJ)], w1[...], preferred_element_type=jnp.float32)
    width = w0.shape[1]
    columns = pl.ds(pl.multiple_of(pl.program_id(0) * width, width), width)
    far = x_ref[lax.rem(j + 1 + c, NJ)]
    total += jnp.dot(far, w2[:, columns], preferred_element_type=jnp.float32)
    for n in range(NQ):
        out_ref[n] = total[n * OUT : (n + 1) * OUT].astype(jnp.bfloat16)


def prepare_kernel(head, k_ref, v_ref, kv_ref):
    for i in range(NY):
        kv_ref[i, :, :HEAD] = k_ref[...]
        kv_ref[i, :, HEAD:] = v_ref[...]


def vmem():
    return pl.BlockSpec(memory_space=pltpu.VMEM)


def near_core(array):
    return pltpu.with_memory_space_constraint(array, pltpu.VMEM)


def out_here(*shape):
    return pltpu.VMEM(shape, jnp.bfloat16)


def smem():
    return pl.BlockSpec(memory_space=pltpu.SMEM)


def kernel(body, shapes, in_specs, **more):
    outs = [vmem() for _ in shapes] if isinstance(shapes, list) else vmem()
    return pl.pallas_call(body, out_shape=shapes, in_specs=in_specs, out_specs=outs, **more)


def per_device(queries, keys, values, lengths, mlp_owner, out_weight, residual):
    x, y, c = lax.axis_index("x"), lax.axis_index("y"), lax.axis_index("c")
    tp = lax.axis_index("q") * NJ + lax.axis_index("j")
    dc = (x * NY + y) * NC + c
    peer = [(0, 1), (1, 0)]

    around = [
        (k * NJ + i, k * NJ + (i + 1 + k) % NJ) for k in range(NC) for i in range(NJ)
    ]
    turned = lax.ppermute(out_weight, ("c", "j"), around)
    block = pl.BlockSpec((TOK, HEAD), lambda i, head: (0, head[0]))
    kv = pl.pallas_call(
        prepare_kernel,
        out_shape=jax.ShapeDtypeStruct((NY, TOK, COLS), jnp.bfloat16),
        grid_spec=pltpu.PrefetchScalarGridSpec(
            num_scalar_prefetch=1,
            grid=(1,),
            in_specs=[block, block],
            out_specs=pl.BlockSpec((NY, TOK, COLS), lambda i, head: (0, 0, 0)),
        ),
        name="prepare",
    )((tp * HEADS_HERE // GROUP).reshape(1).astype(jnp.int32), keys, values)
    own = lax.all_to_all(kv, "y", 0, 0, tiled=True).reshape(NY * TOK, COLS)
    moved = [lax.ppermute(queries, "x", [(i, i - s) for i in range(s, NX)]) for s in range(1, NX)]
    other = lax.ppermute(own, "c", peer)

    partial = kernel(
        attend_kernel,
        out_here(NX, PART, QROWS),
        [smem()] + [vmem()] * (NX + 2),
        scratch_shapes=[
            pltpu.VMEM((NX, TOK, COLS), jnp.bfloat16),
            pltpu.VMEM((QROWS, HEAD), jnp.bfloat16),
            pltpu.VMEM((1, QROWS), jnp.float32),
            pltpu.VMEM((1, QROWS), jnp.float32),
            pltpu.VMEM((HEAD, QROWS), jnp.float32),
        ],
    )(lengths, *map(near_core, (queries, *moved)), near_core(own), near_core(other))
    parts = lax.all_to_all(partial, "x", 0, 0, tiled=True)

    targets = lax.dynamic_slice_in_dim(mlp_owner, dc * TOK, TOK, 0)
    placement = kernel(place_kernel, out_here(SLOT_TOTAL, TOK), [vmem(), vmem()])(
        targets.reshape(1, TOK), targets.reshape(TOK, 1)
    )
    outgoing = kernel(
        merge_kernel, out_here(SLOT_TOTAL, COLS), [vmem(), vmem()]
    )(near_core(placement), near_core(parts))
    outgoing = outgoing.reshape(N_DC, PADDED, COLS)
    incoming = lax.all_to_all(outgoing, ("x", "y", "c"), 0, 0, tiled=True)
    chooser = kernel(choose_kernel, out_here(TOK, SLOT_TOTAL), [vmem()])(
        mlp_owner.reshape(N_DC, TOK)
    )
    owned = kernel(collect_kernel, out_here(TOK, COLS), [vmem(), vmem()])(
        near_core(chooser), near_core(incoming.reshape(SLOT_TOTAL, COLS))
    )
    turned, _ = lax.optimization_barrier((turned, outgoing))
    swapped = lax.ppermute(turned, "c", peer)
    owned, swapped = lax.optimization_barrier((owned, swapped))
    shared = lax.all_to_all(owned.reshape(NJ, TOK // NJ, COLS), "j", 0, 0, tiled=True)

    width = out_weight.shape[1]
    tile = 1024
    projected = pl.pallas_call(
        project_kernel,
        out_shape=jax.ShapeDtypeStruct((NQ, OUT, width), jnp.bfloat16),
        grid=(width // tile,),
        in_specs=[vmem()] + [pl.BlockSpec((COLS, tile), lambda n: (0, n))] * 2 + [vmem()],
        out_specs=pl.BlockSpec((NQ, OUT, tile), lambda n: (0, 0, n)),
        name="project",
    )(near_core(shared), out_weight, turned, near_core(swapped))
    blocks = lax.all_to_all(projected, "q", 0, 0, tiled=True)
    total = residual.astype(jnp.float32)
    for n in range(NQ):
        total += blocks[n].astype(jnp.float32)
    return total.astype(jnp.bfloat16)


def solution(mesh):
    fine = Mesh(mesh.devices.reshape(NX, NY, NC, NQ, NJ), ("x", "y", "c", "q", "j"))
    dcs, tps = ("x", "y", "c"), ("q", "j")

    return jax.shard_map(
        per_device,
        mesh=fine,
        in_specs=(
            P(dcs, tps),
            P(dcs, None),
            P(dcs, None),
            P(),
            P(),
            P(tps, None),
            P(dcs + tps, None),
        ),
        out_specs=P(dcs + tps, None),
        check_vma=False,
    )
```

```python
import jax
import jax.numpy as jnp
from jax import lax
from jax.experimental import pallas as pl
from jax.experimental.pallas import tpu as pltpu
from jax.sharding import Mesh, PartitionSpec as P

HEAD = 128
GROUP = 4
NX, NY, NC, NQ, NJ = 4, 8, 2, 4, 3
TOK = 192
DOCS = 24
HEADS_HERE = 2
COLS = HEADS_HERE * HEAD
QROWS = HEADS_HERE * TOK
OUT = TOK // (NQ * NJ)
N_DC = NX * NY * NC
PADDED = 8
SLOT_TOTAL = N_DC * PADDED
CHUNK_SLABS = 4
CHUNK = CHUNK_SLABS * TOK
PART = HEAD + 16
LOG2E = 1.4426950408889634
SCALE2 = HEAD**-0.5 * LOG2E
NEG = -1e30
FLOOR = -1e9


SMALL = pltpu.CompilerParams(vmem_limit_bytes=24 << 20)
NT = (((1,), (1,)), ((), ()))
TN = (((0,), (0,)), ((), ()))


def round_up(v):
    return (v + jnp.abs(v) * 0.0079).astype(jnp.bfloat16).astype(jnp.float32)


def attend_kernel(lengths, *refs):
    q_refs, (own_ref, peer_ref, out_ref, q_all, q_s, m_s, l_s, acc_s) = refs[:NX], refs[NX:]
    for s, q_ref in enumerate(q_refs):
        q_all[s] = q_ref[...]
    x, y, c = (lax.axis_index(a) for a in ("x", "y", "c"))

    def empty(xs, carry):
        out_ref[xs, :HEAD, :] = jnp.zeros((HEAD, QROWS), jnp.bfloat16)
        rows = lax.broadcasted_iota(jnp.int32, (PART - HEAD, QROWS), 0)
        out_ref[xs, HEAD:, :] = jnp.where(rows == 0, FLOOR, 0.0).astype(jnp.bfloat16)
        return carry

    lax.fori_loop(0, x, empty, 0)

    def slab(xs, carry):
        p0 = (xs * (NY * NC) + y * NC + c) * TOK
        last = p0 + TOK - 1
        lane = lax.broadcasted_iota(jnp.int32, (1, QROWS), 1)
        pos = p0 + jnp.where(lane >= TOK, lane - TOK, lane)
        start = jnp.zeros((1, QROWS), jnp.int32)
        first_start = jnp.int32(0)
        last_start = jnp.int32(0)
        end = jnp.int32(0)
        for k in range(DOCS):
            end = end + lengths[k]
            start = jnp.where(pos >= end, end, start)
            first_start = jnp.where(p0 >= end, end, first_start)
            last_start = jnp.where(last >= end, end, last_start)
        q_s[:TOK, :] = q_all[xs - x, :, :HEAD]
        q_s[TOK:, :] = q_all[xs - x, :, HEAD:]
        m_s[...] = jnp.full((1, QROWS), FLOOR, jnp.float32)
        l_s[...] = jnp.zeros((1, QROWS), jnp.float32)
        acc_s[...] = jnp.zeros((HEAD, QROWS), jnp.float32)

        def chunk(ch, carry):
            low = (x * NY + ch * CHUNK_SLABS) * NC * TOK
            high = low + CHUNK_SLABS * NC * TOK - 1
            rows = pl.ds(pl.multiple_of(ch * CHUNK, CHUNK), CHUNK)

            def update(masked):
                pieces = []
                for ref, core in ((own_ref, c), (peer_ref, 1 - c)):
                    s = lax.dot_general(
                        ref[rows, :HEAD], q_s[...], NT, preferred_element_type=jnp.float32
                    )
                    s = s * SCALE2
                    if masked:
                        at = lax.broadcasted_iota(jnp.int32, (CHUNK, 1), 0)
                        slab_at = jnp.zeros((CHUNK, 1), jnp.int32)
                        for n in range(1, CHUNK_SLABS):
                            slab_at += (at >= n * TOK).astype(jnp.int32)
                        key_pos = low + core * TOK + at + slab_at * ((NC - 1) * TOK)
                        s = jnp.where((key_pos >= start) & (key_pos <= pos), s, NEG)
                    pieces.append(s)
                m_old = m_s[...]
                top = [jnp.max(s, axis=0, keepdims=True) for s in pieces]
                m_new = jnp.maximum(m_old, round_up(jnp.maximum(top[0], top[1])))
                fix = jnp.exp2(m_old - m_new)
                m_s[...] = m_new
                total = l_s[...] * fix
                mixed = acc_s[...] * fix
                for s, ref in zip(pieces, (own_ref, peer_ref)):
                    w = jnp.exp2(s - m_new)
                    total = total + jnp.sum(w, axis=0, keepdims=True)
                    mixed = mixed + lax.dot_general(
                        ref[rows, HEAD:],
                        w.astype(jnp.bfloat16),
                        TN,
                        preferred_element_type=jnp.float32,
                    )
                l_s[...] = total
                acc_s[...] = mixed

            needed = (low <= last) & (high >= first_start)
            whole = (high <= p0) & (low >= last_start)

            @pl.when(needed & whole)
            def _():
                update(False)

            @pl.when(needed & jnp.logical_not(whole))
            def _():
                update(True)

            return carry

        lax.fori_loop(0, NY // CHUNK_SLABS, chunk, 0)

        out_ref[xs, :HEAD, :] = acc_s[...].astype(jnp.bfloat16)
        total = l_s[...]
        high_part = total.astype(jnp.bfloat16).astype(jnp.float32)
        rows = lax.broadcasted_iota(jnp.int32, (PART - HEAD, QROWS), 0)
        stats = jnp.where(rows == 0, m_s[...], jnp.where(rows == 1, high_part, total - high_part))
        out_ref[xs, HEAD:, :] = stats.astype(jnp.bfloat16)
        return carry

    lax.fori_loop(x, NX, slab, 0)


def place_kernel(row_ref, col_ref, out_ref):
    target = row_ref[...]
    earlier = lax.broadcasted_iota(jnp.int32, (TOK, TOK), 0) < lax.broadcasted_iota(
        jnp.int32, (TOK, TOK), 1
    )
    same = (col_ref[...] == target) & earlier
    rank = jnp.sum(same.astype(jnp.int32), axis=0, keepdims=True)
    slot = target * PADDED + rank
    ids = lax.broadcasted_iota(jnp.int32, (SLOT_TOTAL, TOK), 0)
    out_ref[...] = (ids == slot).astype(jnp.float32).astype(jnp.bfloat16)


def merge_kernel(placement, part_ref, out_ref):
    m = [part_ref[i, HEAD : HEAD + 1, :].astype(jnp.float32) for i in range(NX)]
    top = jnp.maximum(jnp.maximum(m[0], m[1]), jnp.maximum(m[2], m[3]))
    total = jnp.zeros((1, QROWS), jnp.float32)
    mixed = jnp.zeros((HEAD, QROWS), jnp.float32)
    for i in range(NX):
        w = jnp.exp2(m[i] - top)
        part = part_ref[i, HEAD + 1 : HEAD + 2, :].astype(jnp.float32)
        part = part + part_ref[i, HEAD + 2 : HEAD + 3, :].astype(jnp.float32)
        total = total + w * part
        mixed = mixed + w * part_ref[i, :HEAD, :].astype(jnp.float32)
    attention = (mixed / total).astype(jnp.bfloat16)
    for h in range(HEADS_HERE):
        rows = lax.dot_general(
            placement[...],
            attention[:, h * TOK : (h + 1) * TOK],
            NT,
            preferred_element_type=jnp.float32,
        )
        out_ref[:, h * HEAD : (h + 1) * HEAD] = rows.astype(jnp.bfloat16)


def choose_kernel(owner_ref, out_ref):
    x, y, c = (lax.axis_index(a) for a in ("x", "y", "c"))
    mine = (owner_ref[...] == (x * NY + y) * NC + c).astype(jnp.float32).astype(jnp.bfloat16)
    count = lax.dot_general(
        jnp.ones((8, TOK), jnp.bfloat16), mine, NT, preferred_element_type=jnp.float32
    ).astype(jnp.bfloat16)
    before = lax.broadcasted_iota(jnp.int32, (N_DC, N_DC), 0) < lax.broadcasted_iota(
        jnp.int32, (N_DC, N_DC), 1
    )
    first = jnp.dot(
        count, before.astype(jnp.float32).astype(jnp.bfloat16), preferred_element_type=jnp.float32
    ).astype(jnp.bfloat16)
    src = lax.broadcasted_iota(jnp.int32, (N_DC, SLOT_TOTAL), 0)
    slot = lax.broadcasted_iota(jnp.int32, (N_DC, SLOT_TOTAL), 1)
    inside = (slot >= src * PADDED) & (slot < (src + 1) * PADDED)
    spread = inside.astype(jnp.float32).astype(jnp.bfloat16)
    count = jnp.dot(count, spread, preferred_element_type=jnp.float32)[:1]
    first = jnp.dot(first, spread, preferred_element_type=jnp.float32)[:1]
    k = (slot[:1] % PADDED).astype(jnp.float32)
    g = jnp.where(k < count, first + k, -1.0).astype(jnp.int32)
    at = lax.broadcasted_iota(jnp.int32, (TOK, 1), 0)
    part = (at >= 64).astype(jnp.int32) + (at >= 128).astype(jnp.int32)
    within = at - 64 * part
    wanted = ((within // 16) * NJ + part) * 16 + within % 16
    out_ref[...] = (g == wanted).astype(jnp.float32).astype(jnp.bfloat16)


def collect_kernel(chooser, in_ref, out_ref):
    out_ref[...] = jnp.dot(chooser[...], in_ref[...], preferred_element_type=jnp.float32).astype(
        jnp.bfloat16
    )


def project_kernel(x_ref, w0, w1, w2, out_ref):
    c, j = lax.axis_index("c"), lax.axis_index("j")
    total = jnp.dot(x_ref[j], w0[...], preferred_element_type=jnp.float32)
    total += jnp.dot(x_ref[lax.rem(j + 2 - c, NJ)], w1[...], preferred_element_type=jnp.float32)
    width = w0.shape[1]
    columns = pl.ds(pl.multiple_of(pl.program_id(0) * width, width), width)
    far = x_ref[lax.rem(j + 1 + c, NJ)]
    total += jnp.dot(far, w2[...], preferred_element_type=jnp.float32)
    for n in range(NQ):
        out_ref[n, :, columns] = total[n * OUT : (n + 1) * OUT].astype(jnp.bfloat16)


def prepare_kernel(head, k_ref, v_ref, kv_ref):
    for i in range(NY):
        kv_ref[i, :, :HEAD] = k_ref[...]
        kv_ref[i, :, HEAD:] = v_ref[...]


def vmem():
    return pl.BlockSpec(memory_space=pltpu.VMEM)


def near_core(array):
    return pltpu.with_memory_space_constraint(array, pltpu.VMEM)


def out_here(*shape):
    return pltpu.VMEM(shape, jnp.bfloat16)


def smem():
    return pl.BlockSpec(memory_space=pltpu.SMEM)


def kernel(body, shapes, in_specs, **more):
    outs = [vmem() for _ in shapes] if isinstance(shapes, list) else vmem()
    return pl.pallas_call(
        body, out_shape=shapes, in_specs=in_specs, out_specs=outs, compiler_params=SMALL, **more
    )


def per_device(queries, keys, values, lengths, mlp_owner, out_weight, residual):
    x, y, c = lax.axis_index("x"), lax.axis_index("y"), lax.axis_index("c")
    tp = lax.axis_index("q") * NJ + lax.axis_index("j")
    dc = (x * NY + y) * NC + c
    peer = [(0, 1), (1, 0)]

    around = [
        (k * NJ + i, k * NJ + (i + 1 + k) % NJ) for k in range(NC) for i in range(NJ)
    ]
    turned = lax.ppermute(out_weight, ("c", "j"), around)
    block = pl.BlockSpec((TOK, HEAD), lambda i, head: (0, head[0]))
    kv = pl.pallas_call(
        prepare_kernel,
        out_shape=jax.ShapeDtypeStruct((NY, TOK, COLS), jnp.bfloat16),
        grid_spec=pltpu.PrefetchScalarGridSpec(
            num_scalar_prefetch=1,
            grid=(1,),
            in_specs=[block, block],
            out_specs=pl.BlockSpec((NY, TOK, COLS), lambda i, head: (0, 0, 0)),
        ),
        name="prepare",
    )((tp * HEADS_HERE // GROUP).reshape(1).astype(jnp.int32), keys, values)
    own = lax.all_to_all(kv, "y", 0, 0, tiled=True).reshape(NY * TOK, COLS)
    moved = [lax.ppermute(queries, "x", [(i, i - s) for i in range(s, NX)]) for s in range(1, NX)]
    other = lax.ppermute(own, "c", peer)

    partial = kernel(
        attend_kernel,
        out_here(NX, PART, QROWS),
        [smem()] + [vmem()] * (NX + 2),
        scratch_shapes=[
            pltpu.VMEM((NX, TOK, COLS), jnp.bfloat16),
            pltpu.VMEM((QROWS, HEAD), jnp.bfloat16),
            pltpu.VMEM((1, QROWS), jnp.float32),
            pltpu.VMEM((1, QROWS), jnp.float32),
            pltpu.VMEM((HEAD, QROWS), jnp.float32),
        ],
    )(lengths, *map(near_core, (queries, *moved)), near_core(own), near_core(other))
    parts = lax.all_to_all(partial, "x", 0, 0, tiled=True)

    targets = lax.dynamic_slice_in_dim(mlp_owner, dc * TOK, TOK, 0)
    placement = kernel(place_kernel, out_here(SLOT_TOTAL, TOK), [vmem(), vmem()])(
        targets.reshape(1, TOK), targets.reshape(TOK, 1)
    )
    outgoing = kernel(
        merge_kernel, out_here(SLOT_TOTAL, COLS), [vmem(), vmem()]
    )(near_core(placement), near_core(parts))
    outgoing = outgoing.reshape(N_DC, PADDED, COLS)
    incoming = lax.all_to_all(outgoing, ("x", "y", "c"), 0, 0, tiled=True)
    chooser = kernel(choose_kernel, out_here(TOK, SLOT_TOTAL), [vmem()])(
        mlp_owner.reshape(N_DC, TOK)
    )
    owned = kernel(collect_kernel, out_here(TOK, COLS), [vmem(), vmem()])(
        near_core(chooser), near_core(incoming.reshape(SLOT_TOTAL, COLS))
    )
    turned, _ = lax.optimization_barrier((turned, outgoing))
    swapped = lax.ppermute(turned, "c", peer)
    owned, swapped = lax.optimization_barrier((owned, swapped))
    shared = lax.all_to_all(owned.reshape(NJ, TOK // NJ, COLS), "j", 0, 0, tiled=True)

    width = out_weight.shape[1]
    tile = 2048
    projected = pl.pallas_call(
        project_kernel,
        out_shape=out_here(NQ, OUT, width),
        grid=(width // tile,),
        in_specs=[vmem()] + [pl.BlockSpec((COLS, tile), lambda n: (0, n))] * 3,
        out_specs=vmem(),
        name="project",
        compiler_params=SMALL,
    )(near_core(shared), out_weight, turned, swapped)
    blocks = lax.all_to_all(projected, "q", 0, 0, tiled=True)
    total = residual.astype(jnp.float32)
    for n in range(NQ):
        total += blocks[n].astype(jnp.float32)
    return total.astype(jnp.bfloat16)


def solution(mesh):
    fine = Mesh(mesh.devices.reshape(NX, NY, NC, NQ, NJ), ("x", "y", "c", "q", "j"))
    dcs, tps = ("x", "y", "c"), ("q", "j")

    return jax.shard_map(
        per_device,
        mesh=fine,
        in_specs=(
            P(dcs, tps),
            P(dcs, None),
            P(dcs, None),
            P(),
            P(),
            P(tps, None),
            P(dcs + tps, None),
        ),
        out_specs=P(dcs + tps, None),
        check_vma=False,
    )
```

```python
import functools

import jax
import jax.numpy as jnp
from jax import lax
from jax.experimental import pallas as pl
from jax.experimental.pallas import tpu as pltpu
from jax.sharding import Mesh, PartitionSpec as P

HEAD = 128
GROUP = 4
NX, NY, NC, NQ, NJ = 4, 8, 2, 4, 3
TOK = 192
DOCS = 24
HEADS_HERE = 2
COLS = HEADS_HERE * HEAD
QROWS = HEADS_HERE * TOK
OUT = TOK // (NQ * NJ)
N_DC = NX * NY * NC
PADDED = 8
SLOT_TOTAL = N_DC * PADDED
CHUNK_SLABS = 4
CHUNK = CHUNK_SLABS * TOK
PART = HEAD + 16
LOG2E = 1.4426950408889634
SCALE2 = HEAD**-0.5 * LOG2E
NEG = -1e30
FLOOR = -1e9


SMALL = pltpu.CompilerParams(vmem_limit_bytes=24 << 20)
NT = (((1,), (1,)), ((), ()))
TN = (((0,), (0,)), ((), ()))


def round_up(v):
    return (v + jnp.abs(v) * 0.0079).astype(jnp.bfloat16).astype(jnp.float32)


def attend_kernel(first, count, lengths, *refs):
    q_refs, (own_ref, peer_ref), rest = refs[:count], refs[count : count + 2], refs[count + 2 :]
    out_refs, (q_all, q_s, m_s, l_s, acc_s) = rest[:count], rest[count:]
    for s, q_ref in enumerate(q_refs):
        q_all[s] = q_ref[...]
    x, y, c = (lax.axis_index(a) for a in ("x", "y", "c"))

    def slab(xs, carry):
        p0 = (xs * (NY * NC) + y * NC + c) * TOK
        last = p0 + TOK - 1
        lane = lax.broadcasted_iota(jnp.int32, (1, QROWS), 1)
        pos = p0 + jnp.where(lane >= TOK, lane - TOK, lane)
        start = jnp.zeros((1, QROWS), jnp.int32)
        first_start = jnp.int32(0)
        last_start = jnp.int32(0)
        end = jnp.int32(0)
        for k in range(DOCS):
            end = end + lengths[k]
            start = jnp.where(pos >= end, end, start)
            first_start = jnp.where(p0 >= end, end, first_start)
            last_start = jnp.where(last >= end, end, last_start)
        q_s[:TOK, :] = q_all[xs - x - first, :, :HEAD]
        q_s[TOK:, :] = q_all[xs - x - first, :, HEAD:]
        m_s[...] = jnp.full((1, QROWS), FLOOR, jnp.float32)
        l_s[...] = jnp.zeros((1, QROWS), jnp.float32)
        acc_s[...] = jnp.zeros((HEAD, QROWS), jnp.float32)

        def chunk(ch, carry):
            low = (x * NY + ch * CHUNK_SLABS) * NC * TOK
            high = low + CHUNK_SLABS * NC * TOK - 1
            rows = pl.ds(pl.multiple_of(ch * CHUNK, CHUNK), CHUNK)

            def update(masked):
                pieces = []
                for ref, core in ((own_ref, c), (peer_ref, 1 - c)):
                    s = lax.dot_general(
                        ref[rows, :HEAD], q_s[...], NT, preferred_element_type=jnp.float32
                    )
                    s = s * SCALE2
                    if masked:
                        at = lax.broadcasted_iota(jnp.int32, (CHUNK, 1), 0)
                        slab_at = jnp.zeros((CHUNK, 1), jnp.int32)
                        for n in range(1, CHUNK_SLABS):
                            slab_at += (at >= n * TOK).astype(jnp.int32)
                        key_pos = low + core * TOK + at + slab_at * ((NC - 1) * TOK)
                        s = jnp.where((key_pos >= start) & (key_pos <= pos), s, NEG)
                    pieces.append(s)
                m_old = m_s[...]
                top = [jnp.max(s, axis=0, keepdims=True) for s in pieces]
                m_new = jnp.maximum(m_old, round_up(jnp.maximum(top[0], top[1])))
                fix = jnp.exp2(m_old - m_new)
                m_s[...] = m_new
                total = l_s[...] * fix
                mixed = acc_s[...] * fix
                for s, ref in zip(pieces, (own_ref, peer_ref)):
                    w = jnp.exp2(s - m_new)
                    total = total + jnp.sum(w, axis=0, keepdims=True)
                    mixed = mixed + lax.dot_general(
                        ref[rows, HEAD:],
                        w.astype(jnp.bfloat16),
                        TN,
                        preferred_element_type=jnp.float32,
                    )
                l_s[...] = total
                acc_s[...] = mixed

            needed = (low <= last) & (high >= first_start)
            whole = (high <= p0) & (low >= last_start)

            @pl.when(needed & whole)
            def _():
                update(False)

            @pl.when(needed & jnp.logical_not(whole))
            def _():
                update(True)

            return carry

        lax.fori_loop(0, NY // CHUNK_SLABS, chunk, 0)

        total = l_s[...]
        high_part = total.astype(jnp.bfloat16).astype(jnp.float32)
        rows = lax.broadcasted_iota(jnp.int32, (PART - HEAD, QROWS), 0)
        stats = jnp.where(rows == 0, m_s[...], jnp.where(rows == 1, high_part, total - high_part))
        for n, out_ref in enumerate(out_refs):

            @pl.when(xs - x - first == n)
            def _(out_ref=out_ref):
                out_ref[:HEAD, :] = acc_s[...].astype(jnp.bfloat16)
                out_ref[HEAD:, :] = stats.astype(jnp.bfloat16)

        return carry

    lax.fori_loop(x + first, jnp.minimum(x + first + count, NX), slab, 0)


def place_kernel(row_ref, col_ref, out_ref):
    target = row_ref[...]
    earlier = lax.broadcasted_iota(jnp.int32, (TOK, TOK), 0) < lax.broadcasted_iota(
        jnp.int32, (TOK, TOK), 1
    )
    same = (col_ref[...] == target) & earlier
    rank = jnp.sum(same.astype(jnp.int32), axis=0, keepdims=True)
    slot = target * PADDED + rank
    ids = lax.broadcasted_iota(jnp.int32, (SLOT_TOTAL, TOK), 0)
    out_ref[...] = (ids == slot).astype(jnp.float32).astype(jnp.bfloat16)


def merge_kernel(placement, *refs):
    part_refs, out_ref = refs[:NX], refs[NX]
    x = lax.axis_index("x")
    m = []
    for s, ref in enumerate(part_refs):
        m.append(jnp.where(s <= x, ref[HEAD : HEAD + 1, :].astype(jnp.float32), FLOOR))
    top = jnp.maximum(jnp.maximum(m[0], m[1]), jnp.maximum(m[2], m[3]))
    total = jnp.zeros((1, QROWS), jnp.float32)
    mixed = jnp.zeros((HEAD, QROWS), jnp.float32)
    for s, ref in enumerate(part_refs):
        w = jnp.exp2(m[s] - top)
        part = ref[HEAD + 1 : HEAD + 2, :].astype(jnp.float32)
        part = part + ref[HEAD + 2 : HEAD + 3, :].astype(jnp.float32)
        total = total + w * part
        mixed = mixed + w * ref[:HEAD, :].astype(jnp.float32)
    attention = (mixed / total).astype(jnp.bfloat16)
    for h in range(HEADS_HERE):
        rows = lax.dot_general(
            placement[...],
            attention[:, h * TOK : (h + 1) * TOK],
            NT,
            preferred_element_type=jnp.float32,
        )
        out_ref[:, h * HEAD : (h + 1) * HEAD] = rows.astype(jnp.bfloat16)


def choose_kernel(owner_ref, out_ref):
    x, y, c = (lax.axis_index(a) for a in ("x", "y", "c"))
    mine = (owner_ref[...] == (x * NY + y) * NC + c).astype(jnp.float32).astype(jnp.bfloat16)
    count = lax.dot_general(
        jnp.ones((8, TOK), jnp.bfloat16), mine, NT, preferred_element_type=jnp.float32
    ).astype(jnp.bfloat16)
    before = lax.broadcasted_iota(jnp.int32, (N_DC, N_DC), 0) < lax.broadcasted_iota(
        jnp.int32, (N_DC, N_DC), 1
    )
    first = jnp.dot(
        count, before.astype(jnp.float32).astype(jnp.bfloat16), preferred_element_type=jnp.float32
    ).astype(jnp.bfloat16)
    src = lax.broadcasted_iota(jnp.int32, (N_DC, SLOT_TOTAL), 0)
    slot = lax.broadcasted_iota(jnp.int32, (N_DC, SLOT_TOTAL), 1)
    inside = (slot >= src * PADDED) & (slot < (src + 1) * PADDED)
    spread = inside.astype(jnp.float32).astype(jnp.bfloat16)
    count = jnp.dot(count, spread, preferred_element_type=jnp.float32)[:1]
    first = jnp.dot(first, spread, preferred_element_type=jnp.float32)[:1]
    k = (slot[:1] % PADDED).astype(jnp.float32)
    g = jnp.where(k < count, first + k, -1.0).astype(jnp.int32)
    at = lax.broadcasted_iota(jnp.int32, (TOK, 1), 0)
    part = (at >= 64).astype(jnp.int32) + (at >= 128).astype(jnp.int32)
    within = at - 64 * part
    wanted = ((within // 16) * NJ + part) * 16 + within % 16
    out_ref[...] = (g == wanted).astype(jnp.float32).astype(jnp.bfloat16)


def collect_kernel(chooser, in_ref, out_ref):
    out_ref[...] = jnp.dot(chooser[...], in_ref[...], preferred_element_type=jnp.float32).astype(
        jnp.bfloat16
    )


def project_kernel(x_ref, w0, w1, w2, out_ref):
    c, j = lax.axis_index("c"), lax.axis_index("j")
    total = jnp.dot(x_ref[j], w0[...], preferred_element_type=jnp.float32)
    total += jnp.dot(x_ref[lax.rem(j + 2 - c, NJ)], w1[...], preferred_element_type=jnp.float32)
    width = w0.shape[1]
    columns = pl.ds(pl.multiple_of(pl.program_id(0) * width, width), width)
    far = x_ref[lax.rem(j + 1 + c, NJ)]
    total += jnp.dot(far, w2[...], preferred_element_type=jnp.float32)
    for n in range(NQ):
        out_ref[n, :, columns] = total[n * OUT : (n + 1) * OUT].astype(jnp.bfloat16)


def prepare_kernel(head, k_ref, v_ref, kv_ref):
    for i in range(NY):
        kv_ref[i, :, :HEAD] = k_ref[...]
        kv_ref[i, :, HEAD:] = v_ref[...]


def vmem():
    return pl.BlockSpec(memory_space=pltpu.VMEM)


def near_core(array):
    return pltpu.with_memory_space_constraint(array, pltpu.VMEM)


def out_here(*shape):
    return pltpu.VMEM(shape, jnp.bfloat16)


def smem():
    return pl.BlockSpec(memory_space=pltpu.SMEM)


def kernel(body, shapes, in_specs, **more):
    outs = [vmem() for _ in shapes] if isinstance(shapes, list) else vmem()
    return pl.pallas_call(
        body, out_shape=shapes, in_specs=in_specs, out_specs=outs, compiler_params=SMALL, **more
    )


def per_device(queries, keys, values, lengths, mlp_owner, out_weight, residual):
    x, y, c = lax.axis_index("x"), lax.axis_index("y"), lax.axis_index("c")
    tp = lax.axis_index("q") * NJ + lax.axis_index("j")
    dc = (x * NY + y) * NC + c
    peer = [(0, 1), (1, 0)]

    around = [
        (k * NJ + i, k * NJ + (i + 1 + k) % NJ) for k in range(NC) for i in range(NJ)
    ]
    turned = lax.ppermute(out_weight, ("c", "j"), around)
    block = pl.BlockSpec((TOK, HEAD), lambda i, head: (0, head[0]))
    kv = pl.pallas_call(
        prepare_kernel,
        out_shape=jax.ShapeDtypeStruct((NY, TOK, COLS), jnp.bfloat16),
        grid_spec=pltpu.PrefetchScalarGridSpec(
            num_scalar_prefetch=1,
            grid=(1,),
            in_specs=[block, block],
            out_specs=pl.BlockSpec((NY, TOK, COLS), lambda i, head: (0, 0, 0)),
        ),
        name="prepare",
    )((tp * HEADS_HERE // GROUP).reshape(1).astype(jnp.int32), keys, values)
    own = lax.all_to_all(kv, "y", 0, 0, tiled=True).reshape(NY * TOK, COLS)
    moved = [lax.ppermute(queries, "x", [(i, i - s) for i in range(s, NX)]) for s in range(1, NX)]
    other = lax.ppermute(own, "c", peer)

    def attend(first, sent):
        return kernel(
            functools.partial(attend_kernel, first, len(sent)),
            [out_here(PART, QROWS)] * len(sent),
            [smem()] + [vmem()] * (len(sent) + 2),
            scratch_shapes=[
                pltpu.VMEM((len(sent), TOK, COLS), jnp.bfloat16),
                pltpu.VMEM((QROWS, HEAD), jnp.bfloat16),
                pltpu.VMEM((1, QROWS), jnp.float32),
                pltpu.VMEM((1, QROWS), jnp.float32),
                pltpu.VMEM((HEAD, QROWS), jnp.float32),
            ],
        )(lengths, *map(near_core, (*sent, own, other)))

    away = attend(1, moved)
    arrived = [
        lax.ppermute(p, "x", [(i, i + s) for i in range(NX - s)]) for s, p in enumerate(away, 1)
    ]
    home = attend(0, [queries])

    targets = lax.dynamic_slice_in_dim(mlp_owner, dc * TOK, TOK, 0)
    placement = kernel(place_kernel, out_here(SLOT_TOTAL, TOK), [vmem(), vmem()])(
        targets.reshape(1, TOK), targets.reshape(TOK, 1)
    )
    outgoing = kernel(
        merge_kernel, out_here(SLOT_TOTAL, COLS), [vmem()] * (NX + 1)
    )(*map(near_core, (placement, *home, *arrived)))
    outgoing = outgoing.reshape(N_DC, PADDED, COLS)
    incoming = lax.all_to_all(outgoing, ("x", "y", "c"), 0, 0, tiled=True)
    chooser = kernel(choose_kernel, out_here(TOK, SLOT_TOTAL), [vmem()])(
        mlp_owner.reshape(N_DC, TOK)
    )
    owned = kernel(collect_kernel, out_here(TOK, COLS), [vmem(), vmem()])(
        near_core(chooser), near_core(incoming.reshape(SLOT_TOTAL, COLS))
    )
    turned, _ = lax.optimization_barrier((turned, outgoing))
    swapped = lax.ppermute(turned, "c", peer)
    owned, swapped = lax.optimization_barrier((owned, swapped))
    shared = lax.all_to_all(owned.reshape(NJ, TOK // NJ, COLS), "j", 0, 0, tiled=True)

    width = out_weight.shape[1]
    tile = 2048
    projected = pl.pallas_call(
        project_kernel,
        out_shape=out_here(NQ, OUT, width),
        grid=(width // tile,),
        in_specs=[vmem()] + [pl.BlockSpec((COLS, tile), lambda n: (0, n))] * 3,
        out_specs=vmem(),
        name="project",
        compiler_params=SMALL,
    )(near_core(shared), out_weight, turned, swapped)
    blocks = lax.all_to_all(projected, "q", 0, 0, tiled=True)
    total = residual.astype(jnp.float32)
    for n in range(NQ):
        total += blocks[n].astype(jnp.float32)
    return total.astype(jnp.bfloat16)


def solution(mesh):
    fine = Mesh(mesh.devices.reshape(NX, NY, NC, NQ, NJ), ("x", "y", "c", "q", "j"))
    dcs, tps = ("x", "y", "c"), ("q", "j")

    return jax.shard_map(
        per_device,
        mesh=fine,
        in_specs=(
            P(dcs, tps),
            P(dcs, None),
            P(dcs, None),
            P(),
            P(),
            P(tps, None),
            P(dcs + tps, None),
        ),
        out_specs=P(dcs + tps, None),
        check_vma=False,
    )
```

```python
import functools

import jax
import jax.numpy as jnp
from jax import lax
from jax.experimental import pallas as pl
from jax.experimental.pallas import tpu as pltpu
from jax.sharding import Mesh, PartitionSpec as P

HEAD = 128
GROUP = 4
NX, NY, NC, NQ, NJ = 4, 8, 2, 4, 3
TOK = 192
DOCS = 24
HEADS_HERE = 2
COLS = HEADS_HERE * HEAD
QROWS = HEADS_HERE * TOK
OUT = TOK // (NQ * NJ)
N_DC = NX * NY * NC
PADDED = 8
SLOT_TOTAL = N_DC * PADDED
CHUNK_SLABS = 4
CHUNK = CHUNK_SLABS * TOK
PART = HEAD + 16
LOG2E = 1.4426950408889634
SCALE2 = HEAD**-0.5 * LOG2E
NEG = -1e30
FLOOR = -1e9


SMALL = pltpu.CompilerParams(vmem_limit_bytes=24 << 20)
NT = (((1,), (1,)), ((), ()))
TN = (((0,), (0,)), ((), ()))


def round_up(v):
    return (v + jnp.abs(v) * 0.0079).astype(jnp.bfloat16).astype(jnp.float32)


def attend_group(lengths, slabs, q_refs, own_ref, peer_ref, out_refs, q_s, m_s, l_s, acc_s):
    x, c = lax.axis_index("x"), lax.axis_index("c")
    count = len(slabs)
    info = []
    for n, (at_slab, q_ref) in enumerate(zip(slabs, q_refs)):
        p0 = at_slab * TOK
        last = p0 + TOK - 1
        lane = lax.broadcasted_iota(jnp.int32, (1, QROWS), 1)
        pos = p0 + jnp.where(lane >= TOK, lane - TOK, lane)
        start = jnp.zeros((1, QROWS), jnp.int32)
        first_start = jnp.int32(0)
        last_start = jnp.int32(0)
        end = jnp.int32(0)
        for k in range(DOCS):
            end = end + lengths[k]
            start = jnp.where(pos >= end, end, start)
            first_start = jnp.where(p0 >= end, end, first_start)
            last_start = jnp.where(last >= end, end, last_start)
        info.append((p0, last, pos, start, first_start, last_start))
        q_s[n * QROWS : n * QROWS + TOK, :] = q_ref[:, :HEAD]
        q_s[n * QROWS + TOK : (n + 1) * QROWS, :] = q_ref[:, HEAD:]
    lanes = count * QROWS
    m_s[:, :lanes] = jnp.full((1, lanes), FLOOR, jnp.float32)
    l_s[:, :lanes] = jnp.zeros((1, lanes), jnp.float32)
    acc_s[:, :lanes] = jnp.zeros((HEAD, lanes), jnp.float32)

    def chunk(ch, carry):
        low = (x * NY + ch * CHUNK_SLABS) * NC * TOK
        high = low + CHUNK_SLABS * NC * TOK - 1
        rows = pl.ds(pl.multiple_of(ch * CHUNK, CHUNK), CHUNK)

        def update(here, pos=None, start=None):
            pieces = []
            for ref, core in ((own_ref, c), (peer_ref, 1 - c)):
                s = lax.dot_general(
                    ref[rows, :HEAD], q_s[here, :], NT, preferred_element_type=jnp.float32
                )
                s = s * SCALE2
                if pos is not None:
                    at = lax.broadcasted_iota(jnp.int32, (CHUNK, 1), 0)
                    slab_at = jnp.zeros((CHUNK, 1), jnp.int32)
                    for n in range(1, CHUNK_SLABS):
                        slab_at += (at >= n * TOK).astype(jnp.int32)
                    key_pos = low + core * TOK + at + slab_at * ((NC - 1) * TOK)
                    s = jnp.where((key_pos >= start) & (key_pos <= pos), s, NEG)
                pieces.append(s)
            m_old = m_s[:, here]
            top = [jnp.max(s, axis=0, keepdims=True) for s in pieces]
            m_new = jnp.maximum(m_old, round_up(jnp.maximum(top[0], top[1])))
            fix = jnp.exp2(m_old - m_new)
            m_s[:, here] = m_new
            total = l_s[:, here] * fix
            mixed = acc_s[:, here] * fix
            for s, ref in zip(pieces, (own_ref, peer_ref)):
                w = jnp.exp2(s - m_new)
                total = total + jnp.sum(w, axis=0, keepdims=True)
                mixed = mixed + lax.dot_general(
                    ref[rows, HEAD:],
                    w.astype(jnp.bfloat16),
                    TN,
                    preferred_element_type=jnp.float32,
                )
            l_s[:, here] = total
            acc_s[:, here] = mixed

        flags = []
        together = jnp.bool_(count > 1)
        for p0, last, pos, start, first_start, last_start in info:
            needed = (low <= last) & (high >= first_start)
            whole = (high <= p0) & (low >= last_start)
            flags.append((needed, whole))
            together = together & needed & whole
        if count > 1:

            @pl.when(together)
            def _():
                update(slice(0, lanes))

        for n, (needed, whole) in enumerate(flags):
            here = slice(n * QROWS, (n + 1) * QROWS)
            alone = needed & jnp.logical_not(together)

            @pl.when(alone & whole)
            def _(here=here):
                update(here)

            @pl.when(alone & jnp.logical_not(whole))
            def _(here=here, n=n):
                update(here, info[n][2], info[n][3])

        return carry

    lax.fori_loop(0, NY // CHUNK_SLABS, chunk, 0)

    for n, out_ref in enumerate(out_refs):
        here = slice(n * QROWS, (n + 1) * QROWS)
        out_ref[:HEAD, :] = acc_s[:, here].astype(jnp.bfloat16)
        total = l_s[:, here]
        high_part = total.astype(jnp.bfloat16).astype(jnp.float32)
        rows = lax.broadcasted_iota(jnp.int32, (PART - HEAD, QROWS), 0)
        stats = jnp.where(
            rows == 0, m_s[:, here], jnp.where(rows == 1, high_part, total - high_part)
        )
        out_ref[HEAD:, :] = stats.astype(jnp.bfloat16)


def attend_kernel(first, groups, lengths, *refs):
    count = sum(groups)
    q_refs, key_refs, rest = refs[:count], refs[count : count + 2], refs[count + 2 :]
    out_refs, scratch = rest[:count], rest[count:]
    x, y, c = (lax.axis_index(a) for a in ("x", "y", "c"))
    at = 0
    for size in groups:
        part = slice(at, at + size)
        slabs = [(x + first + n) * (NY * NC) + y * NC + c for n in range(at, at + size)]
        attend_group(lengths, slabs, q_refs[part], *key_refs, out_refs[part], *scratch)
        at += size


def place_kernel(row_ref, col_ref, out_ref):
    target = row_ref[...]
    earlier = lax.broadcasted_iota(jnp.int32, (TOK, TOK), 0) < lax.broadcasted_iota(
        jnp.int32, (TOK, TOK), 1
    )
    same = (col_ref[...] == target) & earlier
    rank = jnp.sum(same.astype(jnp.int32), axis=0, keepdims=True)
    slot = target * PADDED + rank
    ids = lax.broadcasted_iota(jnp.int32, (SLOT_TOTAL, TOK), 0)
    out_ref[...] = (ids == slot).astype(jnp.float32).astype(jnp.bfloat16)


def merge_kernel(placement, *refs):
    part_refs, out_ref = refs[:NX], refs[NX]
    x = lax.axis_index("x")
    m = []
    for s, ref in enumerate(part_refs):
        m.append(jnp.where(s <= x, ref[HEAD : HEAD + 1, :].astype(jnp.float32), FLOOR))
    top = jnp.maximum(jnp.maximum(m[0], m[1]), jnp.maximum(m[2], m[3]))
    total = jnp.zeros((1, QROWS), jnp.float32)
    mixed = jnp.zeros((HEAD, QROWS), jnp.float32)
    for s, ref in enumerate(part_refs):
        w = jnp.exp2(m[s] - top)
        part = ref[HEAD + 1 : HEAD + 2, :].astype(jnp.float32)
        part = part + ref[HEAD + 2 : HEAD + 3, :].astype(jnp.float32)
        total = total + w * part
        mixed = mixed + w * ref[:HEAD, :].astype(jnp.float32)
    attention = (mixed / total).astype(jnp.bfloat16)
    for h in range(HEADS_HERE):
        rows = lax.dot_general(
            placement[...],
            attention[:, h * TOK : (h + 1) * TOK],
            NT,
            preferred_element_type=jnp.float32,
        )
        out_ref[:, h * HEAD : (h + 1) * HEAD] = rows.astype(jnp.bfloat16)


def choose_kernel(owner_ref, out_ref):
    x, y, c = (lax.axis_index(a) for a in ("x", "y", "c"))
    mine = (owner_ref[...] == (x * NY + y) * NC + c).astype(jnp.float32).astype(jnp.bfloat16)
    count = lax.dot_general(
        jnp.ones((8, TOK), jnp.bfloat16), mine, NT, preferred_element_type=jnp.float32
    ).astype(jnp.bfloat16)
    before = lax.broadcasted_iota(jnp.int32, (N_DC, N_DC), 0) < lax.broadcasted_iota(
        jnp.int32, (N_DC, N_DC), 1
    )
    first = jnp.dot(
        count, before.astype(jnp.float32).astype(jnp.bfloat16), preferred_element_type=jnp.float32
    ).astype(jnp.bfloat16)
    src = lax.broadcasted_iota(jnp.int32, (N_DC, SLOT_TOTAL), 0)
    slot = lax.broadcasted_iota(jnp.int32, (N_DC, SLOT_TOTAL), 1)
    inside = (slot >= src * PADDED) & (slot < (src + 1) * PADDED)
    spread = inside.astype(jnp.float32).astype(jnp.bfloat16)
    count = jnp.dot(count, spread, preferred_element_type=jnp.float32)[:1]
    first = jnp.dot(first, spread, preferred_element_type=jnp.float32)[:1]
    k = (slot[:1] % PADDED).astype(jnp.float32)
    g = jnp.where(k < count, first + k, -1.0).astype(jnp.int32)
    at = lax.broadcasted_iota(jnp.int32, (TOK, 1), 0)
    part = (at >= 64).astype(jnp.int32) + (at >= 128).astype(jnp.int32)
    within = at - 64 * part
    wanted = ((within // 16) * NJ + part) * 16 + within % 16
    out_ref[...] = (g == wanted).astype(jnp.float32).astype(jnp.bfloat16)


def collect_kernel(chooser, in_ref, out_ref):
    out_ref[...] = jnp.dot(chooser[...], in_ref[...], preferred_element_type=jnp.float32).astype(
        jnp.bfloat16
    )


def project_kernel(x_ref, w0, w1, w2, out_ref):
    c, j = lax.axis_index("c"), lax.axis_index("j")
    total = jnp.dot(x_ref[j], w0[...], preferred_element_type=jnp.float32)
    total += jnp.dot(x_ref[lax.rem(j + 2 - c, NJ)], w1[...], preferred_element_type=jnp.float32)
    width = w0.shape[1]
    columns = pl.ds(pl.multiple_of(pl.program_id(0) * width, width), width)
    far = x_ref[lax.rem(j + 1 + c, NJ)]
    total += jnp.dot(far, w2[...], preferred_element_type=jnp.float32)
    for n in range(NQ):
        out_ref[n, :, columns] = total[n * OUT : (n + 1) * OUT].astype(jnp.bfloat16)


def prepare_kernel(k_ref, v_ref, kv_ref, sems):
    tp = lax.axis_index("q") * NJ + lax.axis_index("j")
    at = pl.ds(pl.multiple_of(tp * HEADS_HERE // GROUP * HEAD, HEAD), HEAD)
    copies = []
    for i in range(NY):
        for n, ref in enumerate((k_ref, v_ref)):
            to = kv_ref.at[i, :, pl.ds(n * HEAD, HEAD)]
            copies.append(pltpu.make_async_copy(ref.at[:, at], to, sems.at[i, n]))
    for copy in copies:
        copy.start()
    for copy in copies:
        copy.wait()


def vmem():
    return pl.BlockSpec(memory_space=pltpu.VMEM)


def near_core(array):
    return pltpu.with_memory_space_constraint(array, pltpu.VMEM)


def out_here(*shape):
    return pltpu.VMEM(shape, jnp.bfloat16)


def smem():
    return pl.BlockSpec(memory_space=pltpu.SMEM)


def kernel(body, shapes, in_specs, **more):
    outs = [vmem() for _ in shapes] if isinstance(shapes, list) else vmem()
    return pl.pallas_call(
        body, out_shape=shapes, in_specs=in_specs, out_specs=outs, compiler_params=SMALL, **more
    )


def per_device(queries, keys, values, lengths, mlp_owner, out_weight, residual):
    x, y, c = lax.axis_index("x"), lax.axis_index("y"), lax.axis_index("c")
    dc = (x * NY + y) * NC + c
    peer = [(0, 1), (1, 0)]

    around = [
        (k * NJ + i, k * NJ + (i + 1 + k) % NJ) for k in range(NC) for i in range(NJ)
    ]
    turned = lax.ppermute(out_weight, ("c", "j"), around)
    kv = pl.pallas_call(
        prepare_kernel,
        out_shape=jax.ShapeDtypeStruct((NY, TOK, COLS), jnp.bfloat16),
        in_specs=[pl.BlockSpec(memory_space=pltpu.HBM)] * 2,
        out_specs=pl.BlockSpec(memory_space=pltpu.HBM),
        scratch_shapes=[pltpu.SemaphoreType.DMA((NY, 2))],
        name="prepare",
    )(keys, values)
    own = lax.all_to_all(kv, "y", 0, 0, tiled=True).reshape(NY * TOK, COLS)
    moved = [lax.ppermute(queries, "x", [(i, i - s) for i in range(s, NX)]) for s in range(1, NX)]
    other = lax.ppermute(own, "c", peer)

    def attend(first, sent, groups):
        lanes = max(groups) * QROWS
        return kernel(
            functools.partial(attend_kernel, first, groups),
            [out_here(PART, QROWS)] * len(sent),
            [smem()] + [vmem()] * (len(sent) + 2),
            scratch_shapes=[
                pltpu.VMEM((lanes, HEAD), jnp.bfloat16),
                pltpu.VMEM((1, lanes), jnp.float32),
                pltpu.VMEM((1, lanes), jnp.float32),
                pltpu.VMEM((HEAD, lanes), jnp.float32),
            ],
        )(lengths, *map(near_core, (*sent, own, other)))

    away = attend(1, moved, (2, 1))
    arrived = [
        lax.ppermute(p, "x", [(i, i + s) for i in range(NX - s)]) for s, p in enumerate(away, 1)
    ]
    home = attend(0, [queries], (1,))

    targets = lax.dynamic_slice_in_dim(mlp_owner, dc * TOK, TOK, 0)
    placement = kernel(place_kernel, out_here(SLOT_TOTAL, TOK), [vmem(), vmem()])(
        targets.reshape(1, TOK), targets.reshape(TOK, 1)
    )
    outgoing = kernel(
        merge_kernel, out_here(SLOT_TOTAL, COLS), [vmem()] * (NX + 1)
    )(*map(near_core, (placement, *home, *arrived)))
    outgoing = outgoing.reshape(N_DC, PADDED, COLS)
    incoming = lax.all_to_all(outgoing, ("x", "y", "c"), 0, 0, tiled=True)
    chooser = kernel(choose_kernel, out_here(TOK, SLOT_TOTAL), [vmem()])(
        mlp_owner.reshape(N_DC, TOK)
    )
    owned = kernel(collect_kernel, out_here(TOK, COLS), [vmem(), vmem()])(
        near_core(chooser), near_core(incoming.reshape(SLOT_TOTAL, COLS))
    )
    turned, _ = lax.optimization_barrier((turned, outgoing))
    swapped = lax.ppermute(turned, "c", peer)
    owned, swapped = lax.optimization_barrier((owned, swapped))
    shared = lax.all_to_all(owned.reshape(NJ, TOK // NJ, COLS), "j", 0, 0, tiled=True)

    width = out_weight.shape[1]
    tile = 2048
    projected = pl.pallas_call(
        project_kernel,
        out_shape=out_here(NQ, OUT, width),
        grid=(width // tile,),
        in_specs=[vmem()] + [pl.BlockSpec((COLS, tile), lambda n: (0, n))] * 3,
        out_specs=vmem(),
        name="project",
        compiler_params=SMALL,
    )(near_core(shared), out_weight, turned, swapped)
    blocks = lax.all_to_all(projected, "q", 0, 0, tiled=True)
    total = residual.astype(jnp.float32)
    for n in range(NQ):
        total += blocks[n].astype(jnp.float32)
    return total.astype(jnp.bfloat16)


def solution(mesh):
    fine = Mesh(mesh.devices.reshape(NX, NY, NC, NQ, NJ), ("x", "y", "c", "q", "j"))
    dcs, tps = ("x", "y", "c"), ("q", "j")

    return jax.shard_map(
        per_device,
        mesh=fine,
        in_specs=(
            P(dcs, tps),
            P(dcs, None),
            P(dcs, None),
            P(),
            P(),
            P(tps, None),
            P(dcs + tps, None),
        ),
        out_specs=P(dcs + tps, None),
        check_vma=False,
    )
```

```python
import functools

import jax
import jax.numpy as jnp
from jax import lax
from jax.experimental import pallas as pl
from jax.experimental.pallas import tpu as pltpu
from jax.sharding import Mesh, PartitionSpec as P

HEAD = 128
GROUP = 4
NX, NY, NC, NQ, NJ = 4, 8, 2, 4, 3
TOK = 192
DOCS = 24
HEADS_HERE = 2
COLS = HEADS_HERE * HEAD
QROWS = HEADS_HERE * TOK
OUT = TOK // (NQ * NJ)
N_DC = NX * NY * NC
PADDED = 8
SLOT_TOTAL = N_DC * PADDED
CHUNK_SLABS = 4
CHUNK = CHUNK_SLABS * TOK
PART = HEAD + 16
LOG2E = 1.4426950408889634
SCALE2 = HEAD**-0.5 * LOG2E
NEG = -1e30
FLOOR = -1e9


SMALL = pltpu.CompilerParams(vmem_limit_bytes=24 << 20)
NT = (((1,), (1,)), ((), ()))
TN = (((0,), (0,)), ((), ()))


def round_up(v):
    return (v + jnp.abs(v) * 0.0079).astype(jnp.bfloat16).astype(jnp.float32)


def attend_group(lengths, slabs, q_refs, own_ref, peer_ref, out_refs, q_s, m_s, l_s, acc_s):
    x, c = lax.axis_index("x"), lax.axis_index("c")
    count = len(slabs)
    info = []
    for n, (at_slab, q_ref) in enumerate(zip(slabs, q_refs)):
        p0 = at_slab * TOK
        last = p0 + TOK - 1
        lane = lax.broadcasted_iota(jnp.int32, (1, QROWS), 1)
        pos = p0 + jnp.where(lane >= TOK, lane - TOK, lane)
        start = jnp.zeros((1, QROWS), jnp.int32)
        first_start = jnp.int32(0)
        last_start = jnp.int32(0)
        end = jnp.int32(0)
        for k in range(DOCS):
            end = end + lengths[k]
            start = jnp.where(pos >= end, end, start)
            first_start = jnp.where(p0 >= end, end, first_start)
            last_start = jnp.where(last >= end, end, last_start)
        info.append((p0, last, pos, start, first_start, last_start))
        q_s[n * QROWS : n * QROWS + TOK, :] = q_ref[:, :HEAD]
        q_s[n * QROWS + TOK : (n + 1) * QROWS, :] = q_ref[:, HEAD:]
    lanes = count * QROWS
    m_s[:, :lanes] = jnp.full((1, lanes), FLOOR, jnp.float32)
    l_s[:, :lanes] = jnp.zeros((1, lanes), jnp.float32)
    acc_s[:, :lanes] = jnp.zeros((HEAD, lanes), jnp.float32)

    def chunk(ch, carry):
        low = (x * NY + ch * CHUNK_SLABS) * NC * TOK
        high = low + CHUNK_SLABS * NC * TOK - 1
        rows = pl.ds(pl.multiple_of(ch * CHUNK, CHUNK), CHUNK)

        def update(here, pos=None, start=None):
            pieces = []
            for ref, core in ((own_ref, c), (peer_ref, 1 - c)):
                s = lax.dot_general(
                    ref[rows, :HEAD], q_s[here, :], NT, preferred_element_type=jnp.float32
                )
                s = s * SCALE2
                if pos is not None:
                    at = lax.broadcasted_iota(jnp.int32, (CHUNK, 1), 0)
                    slab_at = jnp.zeros((CHUNK, 1), jnp.int32)
                    for n in range(1, CHUNK_SLABS):
                        slab_at += (at >= n * TOK).astype(jnp.int32)
                    key_pos = low + core * TOK + at + slab_at * ((NC - 1) * TOK)
                    s = jnp.where((key_pos >= start) & (key_pos <= pos), s, NEG)
                pieces.append(s)
            m_old = m_s[:, here]
            top = [jnp.max(s, axis=0, keepdims=True) for s in pieces]
            m_new = jnp.maximum(m_old, round_up(jnp.maximum(top[0], top[1])))
            fix = jnp.exp2(m_old - m_new)
            m_s[:, here] = m_new
            total = l_s[:, here] * fix
            mixed = acc_s[:, here] * fix
            for s, ref in zip(pieces, (own_ref, peer_ref)):
                w = jnp.exp2(s - m_new)
                total = total + jnp.sum(w, axis=0, keepdims=True)
                mixed = mixed + lax.dot_general(
                    ref[rows, HEAD:],
                    w.astype(jnp.bfloat16),
                    TN,
                    preferred_element_type=jnp.float32,
                )
            l_s[:, here] = total
            acc_s[:, here] = mixed

        flags = []
        together = jnp.bool_(count > 1)
        for p0, last, pos, start, first_start, last_start in info:
            needed = (low <= last) & (high >= first_start)
            whole = (high <= p0) & (low >= last_start)
            flags.append((needed, whole))
            together = together & needed & whole
        if count > 1:

            @pl.when(together)
            def _():
                update(slice(0, lanes))

        for n, (needed, whole) in enumerate(flags):
            here = slice(n * QROWS, (n + 1) * QROWS)
            alone = needed & jnp.logical_not(together)

            @pl.when(alone & whole)
            def _(here=here):
                update(here)

            @pl.when(alone & jnp.logical_not(whole))
            def _(here=here, n=n):
                update(here, info[n][2], info[n][3])

        return carry

    lax.fori_loop(0, NY // CHUNK_SLABS, chunk, 0)

    for n, out_ref in enumerate(out_refs):
        here = slice(n * QROWS, (n + 1) * QROWS)
        out_ref[:HEAD, :] = acc_s[:, here].astype(jnp.bfloat16)
        total = l_s[:, here]
        high_part = total.astype(jnp.bfloat16).astype(jnp.float32)
        rows = lax.broadcasted_iota(jnp.int32, (PART - HEAD, QROWS), 0)
        stats = jnp.where(
            rows == 0, m_s[:, here], jnp.where(rows == 1, high_part, total - high_part)
        )
        out_ref[HEAD:, :] = stats.astype(jnp.bfloat16)


def attend_kernel(first, groups, lengths, *refs):
    count = sum(groups)
    q_refs, key_refs, rest = refs[:count], refs[count : count + 2], refs[count + 2 :]
    out_refs, scratch = rest[:count], rest[count:]
    x, y, c = (lax.axis_index(a) for a in ("x", "y", "c"))
    at = 0
    for size in groups:
        part = slice(at, at + size)
        slabs = [(x + first + n) * (NY * NC) + y * NC + c for n in range(at, at + size)]
        attend_group(lengths, slabs, q_refs[part], *key_refs, out_refs[part], *scratch)
        at += size


def place_kernel(row_ref, col_ref, out_ref):
    target = row_ref[...]
    earlier = lax.broadcasted_iota(jnp.int32, (TOK, TOK), 0) < lax.broadcasted_iota(
        jnp.int32, (TOK, TOK), 1
    )
    same = (col_ref[...] == target) & earlier
    rank = jnp.sum(same.astype(jnp.int32), axis=0, keepdims=True)
    slot = target * PADDED + rank
    ids = lax.broadcasted_iota(jnp.int32, (SLOT_TOTAL, TOK), 0)
    out_ref[...] = (ids == slot).astype(jnp.float32).astype(jnp.bfloat16)


def merge_kernel(placement, *refs):
    part_refs, out_ref = refs[:NX], refs[NX]
    x = lax.axis_index("x")
    m = []
    for s, ref in enumerate(part_refs):
        m.append(jnp.where(s <= x, ref[HEAD : HEAD + 1, :].astype(jnp.float32), FLOOR))
    top = jnp.maximum(jnp.maximum(m[0], m[1]), jnp.maximum(m[2], m[3]))
    total = jnp.zeros((1, QROWS), jnp.float32)
    mixed = jnp.zeros((HEAD, QROWS), jnp.float32)
    for s, ref in enumerate(part_refs):
        w = jnp.exp2(m[s] - top)
        part = ref[HEAD + 1 : HEAD + 2, :].astype(jnp.float32)
        part = part + ref[HEAD + 2 : HEAD + 3, :].astype(jnp.float32)
        total = total + w * part
        mixed = mixed + w * ref[:HEAD, :].astype(jnp.float32)
    attention = (mixed / total).astype(jnp.bfloat16)
    for h in range(HEADS_HERE):
        rows = lax.dot_general(
            placement[...],
            attention[:, h * TOK : (h + 1) * TOK],
            NT,
            preferred_element_type=jnp.float32,
        )
        out_ref[:, h * HEAD : (h + 1) * HEAD] = rows.astype(jnp.bfloat16)


def choose_kernel(owner_ref, out_ref):
    x, y, c = (lax.axis_index(a) for a in ("x", "y", "c"))
    mine = (owner_ref[...] == (x * NY + y) * NC + c).astype(jnp.float32).astype(jnp.bfloat16)
    count = lax.dot_general(
        jnp.ones((8, TOK), jnp.bfloat16), mine, NT, preferred_element_type=jnp.float32
    ).astype(jnp.bfloat16)
    before = lax.broadcasted_iota(jnp.int32, (N_DC, N_DC), 0) < lax.broadcasted_iota(
        jnp.int32, (N_DC, N_DC), 1
    )
    first = jnp.dot(
        count, before.astype(jnp.float32).astype(jnp.bfloat16), preferred_element_type=jnp.float32
    ).astype(jnp.bfloat16)
    src = lax.broadcasted_iota(jnp.int32, (N_DC, SLOT_TOTAL), 0)
    slot = lax.broadcasted_iota(jnp.int32, (N_DC, SLOT_TOTAL), 1)
    inside = (slot >= src * PADDED) & (slot < (src + 1) * PADDED)
    spread = inside.astype(jnp.float32).astype(jnp.bfloat16)
    count = jnp.dot(count, spread, preferred_element_type=jnp.float32)[:1]
    first = jnp.dot(first, spread, preferred_element_type=jnp.float32)[:1]
    k = (slot[:1] % PADDED).astype(jnp.float32)
    g = jnp.where(k < count, first + k, -1.0).astype(jnp.int32)
    at = lax.broadcasted_iota(jnp.int32, (TOK, 1), 0)
    part = (at >= 64).astype(jnp.int32) + (at >= 128).astype(jnp.int32)
    within = at - 64 * part
    wanted = ((within // 16) * NJ + part) * 16 + within % 16
    out_ref[...] = (g == wanted).astype(jnp.float32).astype(jnp.bfloat16)


def collect_kernel(chooser, in_ref, out_ref):
    out_ref[...] = jnp.dot(chooser[...], in_ref[...], preferred_element_type=jnp.float32).astype(
        jnp.bfloat16
    )


def project_kernel(x_ref, w0, w1, w2, out_ref):
    c, j = lax.axis_index("c"), lax.axis_index("j")
    total = jnp.dot(x_ref[j], w0[...], preferred_element_type=jnp.float32)
    total += jnp.dot(x_ref[lax.rem(j + 2 - c, NJ)], w1[...], preferred_element_type=jnp.float32)
    width = w0.shape[1]
    columns = pl.ds(pl.multiple_of(pl.program_id(0) * width, width), width)
    far = x_ref[lax.rem(j + 1 + c, NJ)]
    total += jnp.dot(far, w2[...], preferred_element_type=jnp.float32)
    for n in range(NQ):
        out_ref[n, :, columns] = total[n * OUT : (n + 1) * OUT].astype(jnp.bfloat16)


def prepare_kernel(head, k_ref, v_ref, kv_ref):
    for i in range(NY):
        kv_ref[i, :, :HEAD] = k_ref[...]
        kv_ref[i, :, HEAD:] = v_ref[...]


def vmem():
    return pl.BlockSpec(memory_space=pltpu.VMEM)


def near_core(array):
    return pltpu.with_memory_space_constraint(array, pltpu.VMEM)


def out_here(*shape):
    return pltpu.VMEM(shape, jnp.bfloat16)


def smem():
    return pl.BlockSpec(memory_space=pltpu.SMEM)


def kernel(body, shapes, in_specs, **more):
    outs = [vmem() for _ in shapes] if isinstance(shapes, list) else vmem()
    return pl.pallas_call(
        body, out_shape=shapes, in_specs=in_specs, out_specs=outs, compiler_params=SMALL, **more
    )


def per_device(queries, keys, values, lengths, mlp_owner, out_weight, residual):
    x, y, c = lax.axis_index("x"), lax.axis_index("y"), lax.axis_index("c")
    tp = lax.axis_index("q") * NJ + lax.axis_index("j")
    dc = (x * NY + y) * NC + c
    peer = [(0, 1), (1, 0)]

    around = [
        (k * NJ + i, k * NJ + (i + 1 + k) % NJ) for k in range(NC) for i in range(NJ)
    ]
    turned = lax.ppermute(out_weight, ("c", "j"), around)
    block = pl.BlockSpec((TOK, HEAD), lambda i, head: (0, head[0]))
    kv = pl.pallas_call(
        prepare_kernel,
        out_shape=jax.ShapeDtypeStruct((NY, TOK, COLS), jnp.bfloat16),
        grid_spec=pltpu.PrefetchScalarGridSpec(
            num_scalar_prefetch=1,
            grid=(1,),
            in_specs=[block, block],
            out_specs=pl.BlockSpec((NY, TOK, COLS), lambda i, head: (0, 0, 0)),
        ),
        name="prepare",
    )((tp * HEADS_HERE // GROUP).reshape(1).astype(jnp.int32), keys, values)
    own = lax.all_to_all(kv, "y", 0, 0, tiled=True).reshape(NY * TOK, COLS)
    moved = [lax.ppermute(queries, "x", [(i, i - s) for i in range(s, NX)]) for s in range(1, NX)]
    other = lax.ppermute(own, "c", peer)

    def attend(first, sent, groups):
        lanes = max(groups) * QROWS
        return kernel(
            functools.partial(attend_kernel, first, groups),
            [out_here(PART, QROWS)] * len(sent),
            [smem()] + [vmem()] * (len(sent) + 2),
            scratch_shapes=[
                pltpu.VMEM((lanes, HEAD), jnp.bfloat16),
                pltpu.VMEM((1, lanes), jnp.float32),
                pltpu.VMEM((1, lanes), jnp.float32),
                pltpu.VMEM((HEAD, lanes), jnp.float32),
            ],
        )(lengths, *map(near_core, (*sent, own, other)))

    away = attend(1, moved, (2, 1))
    arrived = [
        lax.ppermute(p, "x", [(i, i + s) for i in range(NX - s)]) for s, p in enumerate(away, 1)
    ]
    home = attend(0, [queries], (1,))

    targets = lax.dynamic_slice_in_dim(mlp_owner, dc * TOK, TOK, 0)
    placement = kernel(place_kernel, out_here(SLOT_TOTAL, TOK), [vmem(), vmem()])(
        targets.reshape(1, TOK), targets.reshape(TOK, 1)
    )
    outgoing = kernel(
        merge_kernel, out_here(SLOT_TOTAL, COLS), [vmem()] * (NX + 1)
    )(*map(near_core, (placement, *home, *arrived)))
    outgoing = outgoing.reshape(N_DC, PADDED, COLS)
    incoming = lax.all_to_all(outgoing, ("x", "y", "c"), 0, 0, tiled=True)
    chooser = kernel(choose_kernel, out_here(TOK, SLOT_TOTAL), [vmem()])(
        mlp_owner.reshape(N_DC, TOK)
    )
    owned = kernel(collect_kernel, out_here(TOK, COLS), [vmem(), vmem()])(
        near_core(chooser), near_core(incoming.reshape(SLOT_TOTAL, COLS))
    )
    turned, _ = lax.optimization_barrier((turned, outgoing))
    swapped = lax.ppermute(turned, "c", peer)
    owned, swapped = lax.optimization_barrier((owned, swapped))
    shared = lax.all_to_all(owned.reshape(NJ, TOK // NJ, COLS), "j", 0, 0, tiled=True)

    width = out_weight.shape[1]
    tile = 2048
    projected = pl.pallas_call(
        project_kernel,
        out_shape=out_here(NQ, OUT, width),
        grid=(width // tile,),
        in_specs=[vmem()] + [pl.BlockSpec((COLS, tile), lambda n: (0, n))] * 3,
        out_specs=vmem(),
        name="project",
        compiler_params=SMALL,
    )(near_core(shared), out_weight, turned, swapped)
    blocks = lax.all_to_all(projected, "q", 0, 0, tiled=True)
    total = residual.astype(jnp.float32)
    for n in range(NQ):
        total += blocks[n].astype(jnp.float32)
    return total.astype(jnp.bfloat16)


def solution(mesh):
    fine = Mesh(mesh.devices.reshape(NX, NY, NC, NQ, NJ), ("x", "y", "c", "q", "j"))
    dcs, tps = ("x", "y", "c"), ("q", "j")

    return jax.shard_map(
        per_device,
        mesh=fine,
        in_specs=(
            P(dcs, tps),
            P(dcs, None),
            P(dcs, None),
            P(),
            P(),
            P(tps, None),
            P(dcs + tps, None),
        ),
        out_specs=P(dcs + tps, None),
        check_vma=False,
    )
```
